32 devices in a mesh: dp: 4 (over x, core), fsdp: 8 (over z, y).
Axes of the slice: x: 2, y: 2, z: 4, core: 2. Of those that a mesh axis runs over, the one named last changes fastest.
Arguments:
- tokens: bfloat16 [98304, 384], P(('dp', 'fsdp')), may hold values from -3 to 3
- cotangent: bfloat16 [98304, 384], P(('dp', 'fsdp')), may hold values from -6 to 6
- image_start: int32 [98304], P(('dp', 'fsdp')), may hold values from 0 to 98303, as said below
- image_end: int32 [98304], P(('dp', 'fsdp')), may hold values from 1 to 98304, as said below
- qkv_weight: bfloat16 [384, 1152], P(('dp', 'fsdp')), may hold values from -2 to 2
- q_bias: bfloat16 [384], P(('dp', 'fsdp')), may hold values from -3 to 3
- v_bias: bfloat16 [384], P(('dp', 'fsdp')), may hold values from -3 to 3
- out_weight: bfloat16 [384, 384], P(('dp', 'fsdp')), may hold values from -4 to 4
- out_bias: bfloat16 [384], P(('dp', 'fsdp')), may hold values from -3 to 3
- up_weight: bfloat16 [384, 1536], P(('dp', 'fsdp')), may hold values from -0.3125 to 0.3125
- up_bias: bfloat16 [1536], P(('dp', 'fsdp')), may hold values from -3 to 3
- down_weight: bfloat16 [1536, 384], P(('dp', 'fsdp')), may hold values from -0.15625 to 0.15625
- down_bias: bfloat16 [384], P(('dp', 'fsdp')), may hold values from -3 to 3
- first_gain: bfloat16 [384], P(('dp', 'fsdp')), may hold values from 0.099609375 to 1.8984375
- first_bias: bfloat16 [384], P(('dp', 'fsdp')), may hold values from -3 to 3
- second_gain: bfloat16 [384], P(('dp', 'fsdp')), may hold values from 0.099609375 to 1.8984375
- second_bias: bfloat16 [384], P(('dp', 'fsdp')), may hold values from -3 to 3
Outputs:
- layer_out: bfloat16 [98304, 384], P(('dp', 'fsdp'))
- input_token_gradient: float32 [98304, 384], P(('dp', 'fsdp'))
- qkv_weight_grad: float32 [384, 1152], P(('dp', 'fsdp'))
- q_bias_grad: float32 [384], P(('dp', 'fsdp'))
- v_bias_grad: float32 [384], P(('dp', 'fsdp'))
- out_weight_grad: float32 [384, 384], P(('dp', 'fsdp'))
- out_bias_grad: float32 [384], P(('dp', 'fsdp'))
- up_weight_grad: float32 [384, 1536], P(('dp', 'fsdp'))
- up_bias_grad: float32 [1536], P(('dp', 'fsdp'))
- down_weight_grad: float32 [1536, 384], P(('dp', 'fsdp'))
- down_bias_grad: float32 [384], P(('dp', 'fsdp'))
- first_gain_grad: float32 [384], P(('dp', 'fsdp'))
- first_bias_grad: float32 [384], P(('dp', 'fsdp'))
- second_gain_grad: float32 [384], P(('dp', 'fsdp'))
- second_bias_grad: float32 [384], P(('dp', 'fsdp'))
The draws below stay inside these ranges and needn't reach their ends.
Inputs may be any that keep to these rules, and one draw needn't show every extreme that they name: Images are runs of consecutive tokens of 98 to 197 tokens each; every boundary between the tokens of two devices (multiples of 3072 inside the stream) lies inside an image of exactly 197 tokens, of which 197 // 4 to 98 lie below the boundary; no other image crosses such a boundary; image_start[t] <= t < image_end[t], and all tokens of an image carry the same two values. `image_end`: see image_start.
All inputs are finite; a program needn't handle non-finite values.
Results may differ from the reference program's by a relative error of at most 0.012.
Values may be sent and summed in bfloat16 or wider, within the bound.
A program may use at most 448 MiB of HBM per device.

```python
import math
import jax
import jax.numpy as jnp
from jax import lax

D = 384
FF = 1536
HEADS = 6
HDIM = 64
SEQ = 197
RIM = 256
TOK_DEV = 3072
TOKENS = 98304


def image_bounds(key):
    shards = TOKENS // TOK_DEV
    below = jax.random.randint(jax.random.fold_in(key, 11), (shards + 1,), SEQ // 4, SEQ // 2 + 1).astype(jnp.int32)
    below = below.at[0].set(0).at[shards].set(0)
    places = jnp.arange(TOKENS, dtype=jnp.int32)
    device = (places // TOK_DEV).astype(jnp.int32)
    offset = (places - device * TOK_DEV).astype(jnp.int32)
    lower_cross = below[device]
    upper_cross = below[device + 1]
    head = jnp.where(device > 0, SEQ - lower_cross, 0).astype(jnp.int32)
    cut = (TOK_DEV - upper_cross).astype(jnp.int32)
    anchor = device * TOK_DEV
    head_begin = anchor - lower_cross
    tail_begin = anchor + TOK_DEV - upper_cross
    spread = jnp.maximum(cut - head, 1).astype(jnp.int32)
    pieces = jnp.maximum(1, (spread + SEQ - 1) // SEQ).astype(jnp.int32)
    inner = jnp.clip(offset - head, 0, spread - 1).astype(jnp.int32)
    which = (((inner + 1) * pieces - 1) // spread).astype(jnp.int32)
    gap_begin = anchor + head + which * spread // pieces
    gap_end = anchor + head + (which + 1) * spread // pieces
    in_head = offset < head
    in_tail = offset >= cut
    begin = jnp.where(in_head, head_begin, jnp.where(in_tail, tail_begin, gap_begin)).astype(jnp.int32)
    finish = jnp.where(in_head, head_begin + SEQ, jnp.where(in_tail, tail_begin + SEQ, gap_end)).astype(jnp.int32)
    return (begin, finish)


def draw_image_start(key, part):
    return image_bounds(key)[0]


def draw_image_end(key, part):
    return image_bounds(key)[1]


def draw_qkv_weight(key, part):
    factor = 1.0 / math.sqrt(D)
    whole = jax.random.normal(key, (D, 3 * D), jnp.float32)
    return jnp.clip(whole * factor, -2.0, 2.0).astype(jnp.bfloat16)


def shard_levels(rng, dims, cuts, least, largest):
    factor_of, own = 1.0, jax.random.fold_in(rng, 6)
    for axis_at, parts in cuts:
        draws = jnp.exp(jax.random.uniform(jax.random.fold_in(own, axis_at), (parts,), jnp.float32, least / len(cuts), largest / len(cuts)))
        factor_of = factor_of * jnp.repeat(draws, dims[axis_at] // parts).reshape([-1 if axis == axis_at else 1 for axis in range(len(dims))])
    return factor_of


def noise(stream_key, extent, scale, most, cuts=(), held_as=jnp.bfloat16):
    entries = jax.random.normal(stream_key, extent, jnp.float32) * scale
    if len(cuts) > 0:
        entries = shard_levels(stream_key, extent, cuts, -0.22, 0.18) * entries
    return jnp.clip(entries, min=-most, max=most).astype(held_as)


def setup_inputs(seed: int = 0) -> dict:
    splits = jax.random.split(jax.random.key(seed), 18)
    tokens = noise(splits[0], (TOKENS, D), 0.5, 3.0, ((0, 32),))
    cotangent = noise(splits[1], (TOKENS, D), 1.0, 6.0, ((0, 32),))
    image_start = draw_image_start(jax.random.fold_in(splits[17], 71), 0)
    image_end = draw_image_end(jax.random.fold_in(splits[17], 71), 0)
    qkv_weight = draw_qkv_weight(jax.random.fold_in(splits[17], 71), 0)
    q_bias = noise(splits[5], (D,), 0.5, 3.0, ((0, 32),))
    v_bias = noise(splits[6], (D,), 0.5, 3.0, ((0, 32),))
    out_weight = noise(splits[7], (D, D), (4 * D // (3 * SEQ)) ** -0.5, 4.0, ((0, 32),))
    out_bias = noise(splits[8], (D,), 0.5, 3.0, ((0, 32),))
    up_weight = noise(splits[9], (D, FF), D ** -0.5, 0.3125, ((0, 32),))
    up_bias = noise(splits[10], (FF,), 0.5, 3.0, ((0, 32),))
    down_weight = noise(splits[11], (FF, D), FF ** -0.5, 0.15625, ((0, 32),))
    down_bias = noise(splits[12], (D,), 0.5, 3.0, ((0, 32),))
    first_gain = jnp.clip(1.0 + 0.18 * jax.random.normal(splits[13], (D,), jnp.float32), 0.099609375, 1.8984375).astype(jnp.bfloat16)
    first_bias = noise(splits[14], (D,), 0.5, 3.0, ((0, 32),))
    second_gain = jnp.clip(1.0 + 0.18 * jax.random.normal(splits[15], (D,), jnp.float32), 0.099609375, 1.8984375).astype(jnp.bfloat16)
    second_bias = noise(splits[16], (D,), 0.5, 3.0, ((0, 32),))
    return dict(tokens=tokens, cotangent=cotangent, image_start=image_start, image_end=image_end, qkv_weight=qkv_weight, q_bias=q_bias, v_bias=v_bias, out_weight=out_weight, out_bias=out_bias, up_weight=up_weight, up_bias=up_bias, down_weight=down_weight, down_bias=down_bias, first_gain=first_gain, first_bias=first_bias, second_gain=second_gain, second_bias=second_bias)


epsilon = 1e-06
masked_score = -1e+30
root_half = 0.7071067811865476
gauss_norm = 0.3989422804014327

def row_layer_norm(rows, gain, shift):
    centre = rows - lax.optimization_barrier(jnp.mean(rows, axis=-1, keepdims=True))
    inverse = lax.rsqrt(lax.optimization_barrier(jnp.mean(centre * centre, axis=-1, keepdims=True)) + epsilon)
    normed = centre * inverse
    return (normed * gain + shift, normed, inverse)

def norm_reverse_pass(grad, normed, inverse, gain):
    scaled = grad * gain
    return inverse * (scaled - lax.optimization_barrier(jnp.mean(scaled, axis=-1, keepdims=True)) - normed * lax.optimization_barrier(jnp.mean(scaled * normed, axis=-1, keepdims=True)))

def gelu_value(pre):
    return 0.5 * pre * (1.0 + lax.erf(pre * root_half))

def gelu_slope(pre):
    return 0.5 * (1.0 + lax.erf(pre * root_half)) + pre * jnp.exp(-0.5 * pre * pre) * gauss_norm

def inner_rows(left, right):
    return jnp.dot(left.T, right, preferred_element_type=jnp.float32)

def block_scores(queries, keys, first_key, end_key, key_pos):
    scores = jnp.einsum('qhd,khd->hqk', queries.astype(jnp.float32), keys.astype(jnp.float32))
    inside = (key_pos[None, :] >= first_key[:, None]) & (key_pos[None, :] < end_key[:, None])
    return jnp.where(inside[None], scores, masked_score)

def reference(tokens, cotangent, image_start, image_end, qkv_weight, q_bias, v_bias, out_weight, out_bias, up_weight, up_bias, down_weight, down_bias, first_gain, first_bias, second_gain, second_bias):
    rows = TOK_DEV
    width = D
    rim = RIM
    block = min(512, rows)
    count = TOKENS // rows
    scale = 1.0 / math.sqrt(HDIM)
    single_precision = jnp.float32
    bf16 = jnp.bfloat16
    leading_gain = first_gain.astype(single_precision)
    leading_bias = first_bias.astype(single_precision)
    trailing_gain = second_gain.astype(single_precision)
    trailing_bias = second_bias.astype(single_precision)
    query_shift = q_bias.astype(single_precision)
    value_shift = jnp.concatenate([jnp.zeros((width,), single_precision), v_bias.astype(single_precision)])
    out_shift = out_bias.astype(single_precision)
    up_shift = up_bias.astype(single_precision)
    down_shift = down_bias.astype(single_precision)
    padded_tokens = jnp.pad(tokens, ((rim, rim), (0, 0)))

    def forward_block(carry, index):
        base = index * rows
        window = lax.dynamic_slice_in_dim(padded_tokens, base, rows + 2 * rim, 0).astype(single_precision)
        normed_w, _, _ = row_layer_norm(window, leading_gain, leading_bias)
        qkv_w = jnp.dot(normed_w.astype(bf16), qkv_weight, preferred_element_type=single_precision)
        key_vals = (qkv_w[:, width:] + value_shift).astype(bf16)
        queries = ((qkv_w[rim:rim + rows, :width] + query_shift) * scale).astype(bf16)
        token_row_matrix = window[rim:rim + rows]
        grad_rows = lax.dynamic_slice_in_dim(cotangent, base, rows, 0)
        first_key = lax.dynamic_slice_in_dim(image_start, base, rows, 0)
        end_key = lax.dynamic_slice_in_dim(image_end, base, rows, 0)
        key_pos = (base - rim + jnp.arange(rows + 2 * rim)).astype(jnp.int32)
        outs = []
        totals = []
        for idx in range(rows // block):
            low = idx * block
            q_blk = queries[low:low + block].reshape(block, HEADS, HDIM)
            span = key_vals[low:low + block + 2 * rim]
            keys = span[:, :width].reshape(-1, HEADS, HDIM)
            values = span[:, width:].reshape(-1, HEADS, HDIM)
            scores = block_scores(q_blk, keys, first_key[low:low + block], end_key[low:low + block], key_pos[low:low + block + 2 * rim])
            top = lax.optimization_barrier(jnp.max(scores, axis=-1, keepdims=True))
            lse = top + jnp.log(lax.optimization_barrier(jnp.sum(jnp.exp(scores - top), axis=-1, keepdims=True)))
            probs_b = jnp.exp(scores - lse).astype(bf16)
            out = jnp.einsum('hqk,khd->qhd', probs_b.astype(single_precision), values.astype(single_precision))
            outs.append(out.reshape(block, width).astype(bf16))
            totals.append(lse)
        attended = jnp.concatenate(outs, axis=0)
        hidden_state = token_row_matrix + jnp.dot(attended, out_weight, preferred_element_type=single_precision) + out_shift
        second_normalized, second_centred_scaled, second_inverse_std = row_layer_norm(hidden_state, trailing_gain, trailing_bias)
        n2 = second_normalized.astype(bf16)
        pre = jnp.dot(n2, up_weight, preferred_element_type=single_precision) + up_shift
        act = gelu_value(pre).astype(bf16)
        layer_rows = (hidden_state + jnp.dot(act, down_weight, preferred_element_type=single_precision) + down_shift).astype(bf16)
        output_grad = grad_rows.astype(single_precision)
        g_down = inner_rows(act, grad_rows)
        g_bdown = lax.optimization_barrier(jnp.sum(output_grad, axis=0))
        d_pre = jnp.dot(grad_rows, down_weight.T, preferred_element_type=single_precision) * gelu_slope(pre)
        d_pre_b = d_pre.astype(bf16)
        g_up = inner_rows(n2, d_pre_b)
        g_bup = lax.optimization_barrier(jnp.sum(d_pre, axis=0))
        second_normed_grad = jnp.dot(d_pre_b, up_weight.T, preferred_element_type=single_precision)
        trailing_gain_grad = lax.optimization_barrier(jnp.sum(second_normed_grad * second_centred_scaled, axis=0))
        g_bias2 = lax.optimization_barrier(jnp.sum(second_normed_grad, axis=0))
        hidden_layer_grad = output_grad + norm_reverse_pass(second_normed_grad, second_centred_scaled, second_inverse_std, trailing_gain)
        d_hid_b = hidden_layer_grad.astype(bf16)
        g_out = inner_rows(attended, d_hid_b)
        g_bout = lax.optimization_barrier(jnp.sum(hidden_layer_grad, axis=0))
        d_att = jnp.dot(d_hid_b, out_weight.T, preferred_element_type=single_precision).astype(bf16)
        key_grad = jnp.zeros((rows + 2 * rim, width), single_precision)
        value_grad = jnp.zeros((rows + 2 * rim, width), single_precision)
        query_grads = []
        for idx in range(rows // block):
            low = idx * block
            q_blk = queries[low:low + block].reshape(block, HEADS, HDIM)
            span = key_vals[low:low + block + 2 * rim]
            keys = span[:, :width].reshape(-1, HEADS, HDIM)
            values = span[:, width:].reshape(-1, HEADS, HDIM)
            scores = block_scores(q_blk, keys, first_key[low:low + block], end_key[low:low + block], key_pos[low:low + block + 2 * rim])
            probs = jnp.exp(scores - totals[idx])
            probs_b = probs.astype(bf16)
            d_out = d_att[low:low + block].reshape(block, HEADS, HDIM)
            value_part = jnp.einsum('hqk,qhd->khd', probs_b.astype(single_precision), d_out.astype(single_precision))
            d_probs = jnp.einsum('qhd,khd->hqk', d_out.astype(single_precision), values.astype(single_precision))
            d_scores = (probs * (d_probs - lax.optimization_barrier(jnp.sum(probs * d_probs, axis=-1, keepdims=True)))).astype(bf16)
            query_part = jnp.einsum('hqk,khd->qhd', d_scores.astype(single_precision), keys.astype(single_precision))
            key_part = jnp.einsum('hqk,qhd->khd', d_scores.astype(single_precision), q_blk.astype(single_precision))
            key_grad = key_grad.at[low:low + block + 2 * rim].add(key_part.reshape(-1, width))
            value_grad = value_grad.at[low:low + block + 2 * rim].add(value_part.reshape(-1, width))
            query_grads.append(query_part.reshape(block, width))
        d_q = jnp.concatenate(query_grads, axis=0) * scale
        g_bq = lax.optimization_barrier(jnp.sum(d_q, axis=0))
        kv_grad = jnp.concatenate([key_grad, value_grad], axis=1)
        new_carry = tuple((a + b for a, b in zip(carry, (g_out, g_bout, g_up, g_bup, g_down, g_bdown, trailing_gain_grad, g_bias2, g_bq))))
        outputs = (layer_rows, hidden_layer_grad, d_q.astype(bf16), kv_grad[rim:rim + rows], kv_grad[:rim], kv_grad[rows + rim:])
        return (new_carry, outputs)
    init = (jnp.zeros((D, D), single_precision), jnp.zeros((D,), single_precision), jnp.zeros((D, FF), single_precision), jnp.zeros((FF,), single_precision), jnp.zeros((FF, D), single_precision), jnp.zeros((D,), single_precision), jnp.zeros((D,), single_precision), jnp.zeros((D,), single_precision), jnp.zeros((D,), single_precision))
    sums, stacked = lax.scan(forward_block, init, jnp.arange(count, dtype=jnp.int32))
    layer_blocks, hid_grads, query_b, own_kv, left_rims, right_rims = stacked
    zero_rim = jnp.zeros((1, rim, 2 * width), single_precision)
    from_prev = jnp.concatenate([zero_rim, right_rims[:-1]], axis=0)
    from_next = jnp.concatenate([left_rims[1:], zero_rim], axis=0)
    token_blocks = tokens.reshape(count, rows, width)

    def second_block(carry, inputs):
        token_row_matrix, hidden_layer_grad, d_q_b, own, prev_rim, next_rim = inputs
        own = own.at[:rim].add(prev_rim)
        own = own.at[rows - rim:].add(next_rim)
        first_normalized, first_centred_scaled, first_inverse_std = row_layer_norm(token_row_matrix.astype(single_precision), leading_gain, leading_bias)
        n1 = first_normalized.astype(bf16)
        d_qkv = jnp.concatenate([d_q_b, own.astype(bf16)], axis=1)
        g_qkv = inner_rows(n1, d_qkv)
        g_bv = lax.optimization_barrier(jnp.sum(own[:, width:], axis=0))
        first_normed_grad = jnp.dot(d_qkv, qkv_weight.T, preferred_element_type=single_precision)
        leading_gain_grad = lax.optimization_barrier(jnp.sum(first_normed_grad * first_centred_scaled, axis=0))
        g_bias1 = lax.optimization_barrier(jnp.sum(first_normed_grad, axis=0))
        token_input_grad = hidden_layer_grad + norm_reverse_pass(first_normed_grad, first_centred_scaled, first_inverse_std, leading_gain)
        new_carry = tuple((a + b for a, b in zip(carry, (g_qkv, g_bv, leading_gain_grad, g_bias1))))
        return (new_carry, token_input_grad)
    init_two = (jnp.zeros((D, 3 * D), single_precision), jnp.zeros((D,), single_precision), jnp.zeros((D,), single_precision), jnp.zeros((D,), single_precision))
    sums_two, token_grads = lax.scan(second_block, init_two, (token_blocks, hid_grads, query_b, own_kv, from_prev, from_next))
    g_out, g_bout, g_up, g_bup, g_down, g_bdown, trailing_gain_grad, g_bias2, g_bq = sums
    g_qkv, g_bv, leading_gain_grad, g_bias1 = sums_two
    return (layer_blocks.reshape(TOKENS, D), token_grads.reshape(TOKENS, D), g_qkv, g_bq, g_bv, g_out, g_bout, g_up, g_bup, g_down, g_bdown, leading_gain_grad, g_bias1, trailing_gain_grad, g_bias2)
```

```python
import functools
import math

import jax
import jax.numpy as jnp
from jax import lax
from jax.experimental import pallas as pl
from jax.experimental.pallas import tpu as pltpu
from jax.sharding import PartitionSpec as P

F32 = jnp.float32
BF16 = jnp.bfloat16
HDIM = 64
EPS = 1e-06
NEG = -1e30
ROOT_HALF = 0.7071067811865476
GAUSS = 0.3989422804014327
LEFT = 112
RIGHT = 160
HALO = LEFT + RIGHT
KEYS = 224
WIN = 256
SHORTEST = 98
AXES = ("dp", "fsdp")
VMEM_BYTES = 63 * 1024 * 1024


def dot(a, b):
    return jnp.dot(a, b, preferred_element_type=F32)


def dot_nt(a, b):
    return lax.dot_general(a, b, (((1,), (1,)), ((), ())), preferred_element_type=F32)


def dot_tn(a, b):
    return lax.dot_general(a, b, (((0,), (0,)), ((), ())), preferred_element_type=F32)


def normed(x):
    centre = x - jnp.mean(x, axis=-1, keepdims=True)
    inverse = lax.rsqrt(jnp.mean(centre * centre, axis=-1, keepdims=True) + EPS)
    return centre * inverse, inverse


def norm_back(grad, xhat, inverse, gain):
    e = grad * gain
    return inverse * (
        e - jnp.mean(e, axis=-1, keepdims=True) - xhat * jnp.mean(e * xhat, axis=-1, keepdims=True)
    )


def colsum(x):
    return jnp.sum(x, axis=0, keepdims=True)


def qkv_rows(rows, weight, gain, shift, bias, width):
    xhat, _ = normed(rows.astype(F32))
    n1 = (xhat * gain + shift).astype(BF16)
    out = dot(n1, weight) + bias
    return jnp.concatenate([out[:, :width] * (1.0 / math.sqrt(HDIM)), out[:, width:]], axis=1).astype(BF16)


def qkv_kernel(tok, tokh, weight, vec, out, outh):
    width = tok.shape[1]
    gain, shift = vec[4:5, :], vec[5:6, :]
    bias = jnp.concatenate([vec[0:1, :], jnp.zeros((1, width), F32), vec[1:2, :]], axis=1)
    out[...] = qkv_rows(tok[...], weight[...], gain, shift, bias, width)

    @pl.when(pl.program_id(0) == pl.num_programs(0) - 1)
    def _():
        outh[...] = qkv_rows(tokh[...], weight[...], gain, shift, bias, width)


def project(tok, tokh, weight, vec):
    rows, width = tok.shape
    tile = 512
    whole = lambda a: pl.BlockSpec(a.shape, lambda i: (0, 0))
    wide = weight.shape[1]
    return pl.pallas_call(
        qkv_kernel,
        grid=(rows // tile,),
        out_shape=(jax.ShapeDtypeStruct((rows, wide), BF16), jax.ShapeDtypeStruct((HALO, wide), BF16)),
        in_specs=[pl.BlockSpec((tile, width), lambda i: (i, 0))] + [whole(a) for a in (tokh, weight, vec)],
        out_specs=(pl.BlockSpec((tile, wide), lambda i: (i, 0)), pl.BlockSpec((HALO, wide), lambda i: (0, 0))),
        name="project",
    )(tok, tokh, weight, vec)


def image_bounds(i, starts, ends):
    s, e = starts[i], ends[i]
    a = pl.multiple_of((s // 16) * 16, 16)
    return s, e, a


def put(ref, a, columns, value, first_row):
    rows = value.shape[0]
    old = ref[pl.ds(a, 16), columns].astype(F32)
    new = value[:16].astype(F32)
    row = lax.broadcasted_iota(jnp.int32, new.shape, 0) + a
    ref[pl.ds(a, 16), columns] = jnp.where(row >= first_row, new, old).astype(ref.dtype)
    ref[pl.ds(a + 16, rows - 16), columns] = value[16:].astype(ref.dtype)


def lane_masks(rows):
    lane = lax.broadcasted_iota(jnp.int32, (rows, 128), 1)
    low = jnp.where(lane < HDIM, 1.0, 0.0)
    return low.astype(BF16), (1.0 - low).astype(BF16)


def attention_forward(i, starts, ends, qkv, probs, att, width):
    s, e, a = image_bounds(i, starts, ends)
    row = lax.broadcasted_iota(jnp.int32, (KEYS, 1), 0) + a
    inside = (row >= s) & (row < e)
    key_bias = jnp.where(inside, 0.0, NEG)
    col = lax.broadcasted_iota(jnp.int32, (1, WIN), 1) + a
    query_on = jnp.where((col >= s) & (col < e), 1.0, 0.0)
    masks = lane_masks(KEYS)
    for pair in range(width // 128):
        lanes = slice(128 * pair, 128 * pair + 128)
        q = qkv[pl.ds(a, WIN), lanes]
        k = qkv[pl.ds(a, KEYS), width + 128 * pair : width + 128 * pair + 128]
        v = qkv[pl.ds(a, KEYS), 2 * width + 128 * pair : 2 * width + 128 * pair + 128]
        total = None
        for half in range(2):
            head = 2 * pair + half
            scores = dot_nt(k * masks[half], q) + key_bias
            top = jnp.max(scores, axis=0, keepdims=True)
            ex = jnp.exp(scores - top)
            p = (ex * (query_on / jnp.sum(ex, axis=0, keepdims=True))).astype(BF16)
            put(probs, a, slice(WIN * head, WIN * head + WIN), p, s)
            part = dot_tn(p, v * masks[half])
            total = part if total is None else total + part
        put(att, a, lanes, total, s)


def attention_backward(i, starts, ends, qkv, probs, att, datt, dqkv, gvec, width, rows):
    s, e, a = image_bounds(i, starts, ends)
    scale = 1.0 / math.sqrt(HDIM)
    row = lax.broadcasted_iota(jnp.int32, (KEYS, 128), 0) + a
    inside = jnp.where((row >= s) & (row < e), 1.0, 0.0).astype(BF16)
    key_masks = [m * inside for m in lane_masks(KEYS)]
    masks = lane_masks(KEYS)
    wide_masks = lane_masks(WIN)
    query = lax.broadcasted_iota(jnp.int32, (WIN, 128), 0) + a
    own = jnp.where((query >= LEFT) & (query < LEFT + rows), 1.0, 0.0)
    group = lax.broadcasted_iota(jnp.int32, (8, width), 1) // HDIM
    heads = jnp.where(group == lax.broadcasted_iota(jnp.int32, (8, width), 0), 1.0, 0.0).astype(BF16)
    both = att[pl.ds(a, WIN), :].astype(F32) * datt[pl.ds(a, WIN), :].astype(F32)
    high = both.astype(BF16)
    delta = dot_nt(heads, high) + dot_nt(heads, (both - high.astype(F32)).astype(BF16))
    for pair in range(width // 128):
        lanes = slice(128 * pair, 128 * pair + 128)
        klanes = slice(width + 128 * pair, width + 128 * pair + 128)
        vlanes = slice(2 * width + 128 * pair, 2 * width + 128 * pair + 128)
        q = qkv[pl.ds(a, WIN), lanes]
        k = qkv[pl.ds(a, KEYS), klanes]
        v = qkv[pl.ds(a, KEYS), vlanes]
        do = datt[pl.ds(a, WIN), lanes]
        dq = dk = dv = None
        for half in range(2):
            head = 2 * pair + half
            p = probs[pl.ds(a, KEYS), WIN * head : WIN * head + WIN]
            dp = dot_nt(v * masks[half], do)
            ds = (p.astype(F32) * (dp - delta[head : head + 1])).astype(BF16)
            dv_part = dot(p, do * wide_masks[half])
            dk_part = dot(ds, q * wide_masks[half])
            dq_part = dot_tn(ds, k * key_masks[half])
            dv = dv_part if dv is None else dv + dv_part
            dk = dk_part if dk is None else dk + dk_part
            dq = dq_part if dq is None else dq + dq_part
        gvec[0:1, lanes] += colsum(dq * own) * scale
        put(dqkv, a, lanes, dq * scale, s)
        put(dqkv, a, klanes, dk, s)
        put(dqkv, a, vlanes, dv, s)


def middle_kernel(
    packs, start_in, end_in, qkv_in, qkvh_in, tok_in, tokh, cot_in, coth, wo, wu, wd, vec, upb,
    out_hbm, dhid_hbm, dqkv_hbm, gvec, gupb, *refs,
):
    if packs:
        packed_hbm, packed, *refs = refs
    gwo, gwu, gwd, qkv, dqkv, probs, att, datt, tok, cot, out_buf, dhid_buf, starts, ends, sems = refs
    rows, width = tok_in.shape
    ff = wu.shape[1]
    extent = rows + HALO
    tile = out_buf.shape[1]
    chunk = 512
    copies = [
        pltpu.make_async_copy(qkvh_in.at[pl.ds(0, LEFT)], qkv.at[pl.ds(0, LEFT)], sems.at[0]),
        pltpu.make_async_copy(qkv_in, qkv.at[pl.ds(LEFT, rows)], sems.at[1]),
        pltpu.make_async_copy(qkvh_in.at[pl.ds(LEFT, RIGHT)], qkv.at[pl.ds(LEFT + rows, RIGHT)], sems.at[2]),
    ]
    later = [
        pltpu.make_async_copy(tok_in, tok, sems.at[3]),
        pltpu.make_async_copy(cot_in, cot, sems.at[4]),
    ]
    for c in copies + later:
        c.start()

    shift = LEFT - lax.axis_index(AXES) * rows
    starts[0] = start_in[0] + shift
    ends[0] = end_in[0] + shift

    def walk(i, n):
        here = ends[i - 1]
        more = here < LEFT + rows
        at = jnp.minimum(here - LEFT, rows - 1)
        starts[i] = here
        ends[i] = end_in[at] + shift
        return jnp.where(more, i + 1, n)

    count = lax.fori_loop(1, starts.shape[0], walk, 1)

    spare = qkv.shape[0] - extent
    qkv[pl.ds(extent, spare), :] = jnp.zeros((spare, qkv.shape[1]), BF16)
    datt[pl.ds(extent, spare), :] = jnp.zeros((spare, width), BF16)
    probs[pl.ds(0, LEFT), :] = jnp.zeros((LEFT, probs.shape[1]), BF16)
    att[pl.ds(0, LEFT), :] = jnp.zeros((LEFT, width), BF16)
    att[pl.ds(LEFT + rows, RIGHT + spare), :] = jnp.zeros((RIGHT + spare, width), BF16)
    dqkv[pl.ds(0, LEFT), :] = jnp.zeros((LEFT, dqkv.shape[1]), BF16)
    for c in copies:
        c.wait()

    @pl.loop(0, count)
    def _(i):
        attention_forward(i, starts, ends, qkv, probs, att, width)

    bo, bd, g2, b2 = (vec[j : j + 1, :] for j in (2, 3, 6, 7))

    def feed(x, c, at, own, sums):
        hid = x.astype(F32) + dot(at, wo[...]) + bo
        xhat, inverse = normed(hid)
        n2 = (xhat * g2 + b2).astype(BF16)
        down = dn2 = None
        if own:
            ct, nt = c.T, n2.T
        for f in range(0, ff, chunk):
            cols = slice(f, f + chunk)
            pre = dot(n2, wu[:, cols]) + upb[0:1, cols]
            half = 0.5 * (1.0 + lax.erf(pre * ROOT_HALF))
            slope = half + pre * jnp.exp(-0.5 * pre * pre) * GAUSS
            dpre = dot_nt(c, wd[cols, :]) * slope
            dpre_b = dpre.astype(BF16)
            part = dot_nt(dpre_b, wu[:, cols])
            dn2 = part if dn2 is None else dn2 + part
            if own:
                act = (pre * half).astype(BF16)
                part = dot(act, wd[cols, :])
                down = part if down is None else down + part
                gwd[:, cols] += dot(ct, act)
                gwu[:, cols] += dot(nt, dpre_b)
                gupb[0:1, cols] += colsum(dpre)
        dhid = c.astype(F32) + norm_back(dn2, xhat, inverse, g2)
        dhid_b = dhid.astype(BF16)
        da = dot_nt(dhid_b, wo[...]).astype(BF16)
        if own:
            gwo[...] += dot_tn(at, dhid_b)
            for j, x in ((2, dhid), (3, c.astype(F32)), (6, dn2 * xhat), (7, dn2)):
                gvec[j : j + 1, :] += colsum(x)
            return hid + down + bd, dhid, da
        return da

    gwo[...] = jnp.zeros_like(gwo)
    gwu[...] = jnp.zeros_like(gwu)
    gwd[...] = jnp.zeros_like(gwd)
    gvec[...] = jnp.zeros_like(gvec)
    gupb[...] = jnp.zeros_like(gupb)
    for c in later:
        c.wait()

    def writes(i, slot):
        at = pl.ds(pl.multiple_of(i * tile, tile), tile)
        return (
            pltpu.make_async_copy(out_buf.at[slot], out_hbm.at[at], sems.at[5 + slot]),
            pltpu.make_async_copy(dhid_buf.at[slot], dhid_hbm.at[at], sems.at[7 + slot]),
        )

    @pl.loop(0, rows // tile)
    def _(i):
        slot = i % 2
        at = pl.multiple_of(i * tile, tile)
        here = pl.ds(pl.multiple_of(LEFT + at, 16), tile)
        layer, dhid, da = feed(tok[pl.ds(at, tile), :], cot[pl.ds(at, tile), :], att[here, :], True, None)
        datt[here, :] = da

        @pl.when(i >= 2)
        def _():
            for w in writes(i - 2, slot):
                w.wait()

        out_buf[slot] = layer.astype(BF16)
        dhid_buf[slot] = dhid
        for w in writes(i, slot):
            w.start()

    sides = jnp.concatenate([att[pl.ds(0, LEFT), :], att[pl.ds(LEFT + rows, RIGHT), :]], axis=0)
    da = feed(tokh[...], coth[...], sides, False, None)
    datt[pl.ds(0, LEFT), :] = da[:LEFT]
    datt[pl.ds(LEFT + rows, RIGHT), :] = da[LEFT:]

    if packs:

        @pl.loop(0, packed.shape[0] // 4)
        def _(i):
            pack_second(i, gwo, gwu, packed)

        pack_down(gwd, packed)
        sent = pltpu.make_async_copy(packed, packed_hbm, sems.at[10])
        sent.start()

    @pl.loop(0, count)
    def _(i):
        attention_backward(i, starts, ends, qkv, probs, att, datt, dqkv, gvec, width, rows)

    last = pltpu.make_async_copy(dqkv.at[pl.ds(LEFT, rows)], dqkv_hbm, sems.at[9])
    last.start()
    n = rows // tile
    for i in range(max(n - 2, 0), n):
        for w in writes(i, i % 2):
            w.wait()
    last.wait()
    if packs:
        sent.wait()


def middle(packs, start, end, qkv, qkvh, tok, tokh, cot, coth, wo, wu, wd, vec, upb):
    rows, width = tok.shape
    ff = wu.shape[1]
    padded = rows + HALO + WIN
    tile = 256
    vmem = pl.BlockSpec(memory_space=pltpu.VMEM)
    smem = pl.BlockSpec(memory_space=pltpu.SMEM)
    anyw = pl.BlockSpec(memory_space=pl.ANY)
    most = rows // SHORTEST + 4
    n = lax.axis_size(AXES)
    S = jax.ShapeDtypeStruct
    sums = [((width, width), F32), ((width, ff), F32), ((width, ff), F32)]
    slabs = (n, 16, SECOND)
    return pl.pallas_call(
        functools.partial(middle_kernel, packs),
        out_shape=[
            S((rows, width), BF16), S((rows, width), F32), S((rows, 3 * width), BF16), S((8, width), F32), S((8, ff), F32),
        ] + ([S(slabs, BF16)] if packs else [S(*a) for a in sums]),
        in_specs=[smem, smem, anyw, anyw, anyw, vmem, anyw, vmem, vmem, vmem, vmem, vmem, vmem],
        out_specs=[anyw, anyw, anyw, vmem, vmem] + ([anyw] if packs else [vmem] * 3),
        scratch_shapes=([pltpu.VMEM(slabs, BF16)] + [pltpu.VMEM(*a) for a in sums] if packs else [])
        + [
            pltpu.VMEM((padded, 3 * width), BF16),
            pltpu.VMEM((padded, 3 * width), BF16),
            pltpu.VMEM((padded, width // HDIM * WIN), BF16),
            pltpu.VMEM((padded, width), BF16),
            pltpu.VMEM((padded, width), BF16),
            pltpu.VMEM((rows, width), BF16),
            pltpu.VMEM((rows, width), BF16),
            pltpu.VMEM((2, tile, width), BF16),
            pltpu.VMEM((2, tile, width), F32),
            pltpu.SMEM((most,), jnp.int32),
            pltpu.SMEM((most,), jnp.int32),
            pltpu.SemaphoreType.DMA((11,)),
        ],
        compiler_params=pltpu.CompilerParams(vmem_limit_bytes=VMEM_BYTES),
        name="middle",
    )(start, end, qkv, qkvh, tok, tokh, cot, coth, wo, wu, wd, vec, upb)


def last_kernel(packs, tok, dhid, dqkv, weight, vec, gvec, gupb, dx, *refs):
    packed, gw, sums = refs if packs else (None,) + refs
    width = tok.shape[1]

    @pl.when(pl.program_id(0) == 0)
    def _():
        gw[...] = jnp.zeros_like(gw)
        sums[...] = gvec[...]

    gain, shift = vec[4:5, :], vec[5:6, :]
    xhat, inverse = normed(tok[...].astype(F32))
    n1 = (xhat * gain + shift).astype(BF16)
    d = dqkv[...]
    gw[...] += dot_tn(n1, d)
    dn1 = dot_nt(d, weight[...])
    sums[1:2, :] += colsum(d[:, 2 * width :].astype(F32))
    sums[4:5, :] += colsum(dn1 * xhat)
    sums[5:6, :] += colsum(dn1)
    dx[...] = dhid[...] + norm_back(dn1, xhat, inverse, gain)

    if packs:

        @pl.when(pl.program_id(0) == pl.num_programs(0) - 1)
        def _():
            @pl.loop(0, packed.shape[0] // 4)
            def _(i):
                pack_first(i, gw, packed)

            pack_small(sums[...], gupb[...], packed)


def last(packs, tok, dhid, dqkv, weight, vec, gvec, gupb):
    rows, width = tok.shape
    wide = weight.shape[1]
    tile = 512
    n = lax.axis_size(AXES)
    whole = lambda a: pl.BlockSpec(a, lambda i: (0,) * len(a))
    rowed = lambda n: pl.BlockSpec((tile, n), lambda i: (i, 0))
    S = jax.ShapeDtypeStruct
    sums = [(width, wide), (8, width)]
    return pl.pallas_call(
        functools.partial(last_kernel, packs),
        grid=(rows // tile,),
        out_shape=[S((rows, width), F32)] + ([S((n, 16, FIRST), BF16)] if packs else [S(a, F32) for a in sums]),
        in_specs=[rowed(width), rowed(width), rowed(wide)] + [whole(a.shape) for a in (weight, vec, gvec, gupb)],
        out_specs=[rowed(width)] + ([whole((n, 16, FIRST))] if packs else [whole(a) for a in sums]),
        scratch_shapes=[pltpu.VMEM(a, F32) for a in sums] if packs else [],
        compiler_params=pltpu.CompilerParams(vmem_limit_bytes=VMEM_BYTES),
        name="last",
    )(tok, dhid, dqkv, weight, vec, gvec, gupb)


COLS, ROWS_UP, LAYERS, CORES = 2, 2, 4, 2
LANES = 3584
SMALL, QKV, OUT, UP, DOWN = 0, 128, 1280, 1664, 2432
PIECES = ((0, 640, 0), (640, 1280, 1), (1280, 2432, 0), (2432, 3584, 1))
MESH = pl.DeviceIdType.MESH


def here():
    dp, fs = lax.axis_index("dp"), lax.axis_index("fsdp")
    return dp // CORES, dp % CORES, fs // ROWS_UP, fs % ROWS_UP


def place(x, c, z, y):
    return (x * CORES + c, z * ROWS_UP + y)


def number(x, c, z, y):
    return (x * CORES + c) * (LAYERS * ROWS_UP) + z * ROWS_UP + y


def greet(ids):
    barrier = pltpu.get_barrier_semaphore()
    for d in ids:
        pl.semaphore_signal(barrier, inc=1, device_id=d, device_id_type=MESH)
    pl.semaphore_wait(barrier, len(ids))


def remote(src, dst, send, recv, to):
    return pltpu.make_async_remote_copy(src_ref=src, dst_ref=dst, send_sem=send, recv_sem=recv, device_id=to, device_id_type=MESH)


def along(step):
    dp, fs = lax.axis_size("dp"), lax.axis_size("fsdp")
    at = lax.rem(lax.axis_index("dp") * fs + lax.axis_index("fsdp") + step + dp * fs, dp * fs)
    return (at // fs, lax.rem(at, fs))


class Gather:
    def __init__(self, slabs, send, recv):
        self.slabs, self.send, self.recv = slabs, send, recv
        self.x, self.c, self.z, self.y = here()

    def copy(self, piece, slab, to):
        lo, hi, _ = PIECES[piece]
        ref = self.slabs.at[slab, :, lo:hi]
        return remote(ref, ref, self.send.at[piece], self.recv.at[piece, slab], to)

    def give(self, piece, slab, axes):
        x, c, z, y = self.x, self.c, self.z, self.y
        for axis in axes:
            if axis == "z":
                for d in range(1, LAYERS):
                    self.copy(piece, slab, place(x, c, lax.rem(z + d, LAYERS), y)).start()
            else:
                to = {"x": place(1 - x, c, z, y), "y": place(x, c, z, 1 - y), "c": place(x, 1 - c, z, y)}[axis]
                self.copy(piece, slab, to).start()

    def own(self, piece):
        self.give(piece, number(self.x, self.c, self.z, self.y), "zxyc")

    def take(self, piece, slab):
        self.copy(piece, slab, place(self.x, self.c, self.z, self.y)).wait_recv()

    def stage(self, piece, level):
        x, c, z, y = self.x, self.c, self.z, self.y
        order = PIECES[piece][2]
        second, third = ("x", "y") if order == 0 else ("y", "x")
        if level == 0:
            group = [(x, lax.rem(z + d, LAYERS), y) for d in range(1, LAYERS)]
            passed = second + third + "c"
        elif level == 1:
            group = [(1 - x, lax.rem(z + d, LAYERS), y) if order == 0 else (x, lax.rem(z + d, LAYERS), 1 - y) for d in range(LAYERS)]
            passed = third + "c"
        else:
            if order == 0:
                group = [(x if s == 0 else 1 - x, lax.rem(z + d, LAYERS), 1 - y) for s in range(2) for d in range(LAYERS)]
            else:
                group = [(1 - x, lax.rem(z + d, LAYERS), y if s == 0 else 1 - y) for s in range(2) for d in range(LAYERS)]
            passed = "c"
        for gx, gz, gy in group:
            slab = number(gx, c, gz, gy)
            self.take(piece, slab)
            self.give(piece, slab, passed)

    def siblings(self, piece):
        x, c, z, y = self.x, self.c, self.z, self.y
        for dx in range(COLS):
            for dy in range(ROWS_UP):
                for d in range(LAYERS):
                    self.take(piece, number(x if dx == 0 else 1 - x, 1 - c, lax.rem(z + d, LAYERS), y if dy == 0 else 1 - y))

    def finish(self, piece):
        lo, hi, _ = PIECES[piece]
        ref = self.slabs.at[pl.ds(0, 31), :, lo:hi]
        remote(ref, ref, self.send.at[piece], self.recv.at[piece, 0], place(self.x, self.c, self.z, self.y)).wait_send()


def gather_kernel(
    small, wqkv_in, wo_in, wu_in, wd_in, tok, cot,
    wqkv, wo, wu, wd, vec, upb, tokh, coth,
    slabs, send, recv, side_send, side_recv,
):
    x, c, z, y = here()
    me = number(x, c, z, y)
    rows, width = tok.shape
    n = slabs.shape[0]
    own = slabs.at[me]
    own[:, SMALL:QKV] = small[...]
    split = 768
    up = wu_in[...].astype(F32)
    top = jnp.concatenate([wqkv_in[...].astype(F32), wo_in[...].astype(F32), up[:, :split]], axis=1)
    rest = jnp.concatenate([up[4 * i : 4 * i + 4, split:] for i in range(3)], axis=1)
    own[:, QKV:DOWN] = jnp.concatenate([top, rest], axis=0).astype(BF16)
    for i in range(3):
        own[:, DOWN + width * i : DOWN + width * (i + 1)] = wd_in[16 * i : 16 * i + 16, :]

    greet(
        [place(x, c, lax.rem(z + d, LAYERS), y) for d in range(1, LAYERS)]
        + [place(1 - x, c, z, y), place(x, c, z, 1 - y), place(x, 1 - c, z, y), along(1), along(-1)]
    )
    g = Gather(slabs, send, recv)
    for p in (0, 1):
        g.own(p)
    sides = []
    for j, (src, dst) in enumerate(((tok, tokh), (cot, coth))):
        sides.append(remote(src.at[pl.ds(rows - LEFT, LEFT)], dst.at[pl.ds(0, LEFT)], side_send.at[2 * j], side_recv.at[2 * j], along(1)))
        sides.append(remote(src.at[pl.ds(0, RIGHT)], dst.at[pl.ds(LEFT, RIGHT)], side_send.at[2 * j + 1], side_recv.at[2 * j + 1], along(-1)))
    for p in (0, 1):
        g.stage(p, 0)
    for p in (2, 3):
        g.own(p)
    for s in sides:
        s.start()
    for level in (1, 2):
        for p in (0, 1):
            g.stage(p, level)
    for level in (0, 1, 2):
        for p in (2, 3):
            g.stage(p, level)
    for p in range(4):
        g.siblings(p)
    for s in sides:
        s.wait()
    for p in range(4):
        g.finish(p)

    @pl.loop(0, n // 4)
    def _(i):
        at = pl.ds(pl.multiple_of(48 * i, 16), 48)
        parts = [slabs[4 * i + d, :, QKV:DOWN].astype(F32) for d in range(4)]
        full = jnp.concatenate([p[:12] for p in parts], axis=0).astype(BF16)
        wqkv[at, :] = full[:, : OUT - QKV]
        wo[at, :] = full[:, OUT - QKV : UP - QKV]
        wu[at, :split] = full[:, UP - QKV :]
        wu[at, split:] = jnp.concatenate([p[12:, split * j : split * (j + 1)] for p in parts for j in range(3)], axis=0).astype(BF16)
        for d in range(4):
            for j in range(3):
                wd[pl.ds(pl.multiple_of(48 * (4 * i + d) + 16 * j, 16), 16), :] = slabs[4 * i + d, :, DOWN + width * j : DOWN + width * (j + 1)]

    lane = lax.broadcasted_iota(jnp.int32, (8, 128), 1)
    lines = [jnp.zeros((8, 128), F32) for _ in range(width // 128)]
    ups = [jnp.zeros((8, 128), F32) for _ in range(upb.shape[1] // 128)]
    for k in range(n):
        s = slabs[k, :, SMALL:QKV].astype(F32)
        for tiles, block, size in ((lines, s[:8], 12), (ups, s[8:], 48)):
            t, by = divmod(size * k, 128)
            moved = pltpu.roll(block, by, 1) if by else block
            if by + size <= 128:
                tiles[t] = tiles[t] + moved
            else:
                tiles[t] = tiles[t] + jnp.where(lane >= by, moved, 0.0)
                tiles[t + 1] = tiles[t + 1] + jnp.where(lane < by, moved, 0.0)
    vec[...] = jnp.concatenate(lines, axis=1)
    upb[...] = jnp.concatenate(ups, axis=1)


def gather_all(small, wqkv, wo, wu, wd, tok, cot):
    n = lax.axis_size(AXES)
    rows, width = tok.shape
    vmem = pl.BlockSpec(memory_space=pltpu.VMEM)
    anyw = pl.BlockSpec(memory_space=pl.ANY)
    S = jax.ShapeDtypeStruct
    return pl.pallas_call(
        gather_kernel,
        out_shape=(
            S((width, wqkv.shape[1]), BF16), S((width, width), BF16), S((width, wu.shape[1]), BF16), S((wd.shape[0] * n, width), BF16),
            S((8, width), F32), S((8, wu.shape[1]), F32), S((HALO, width), BF16), S((HALO, width), BF16),
        ),
        in_specs=[vmem] * 5 + [anyw] * 2,
        out_specs=(vmem,) * 6 + (anyw,) * 2,
        scratch_shapes=[
            pltpu.VMEM((n, 16, LANES), BF16),
            pltpu.SemaphoreType.DMA((4,)),
            pltpu.SemaphoreType.DMA((4, n)),
            pltpu.SemaphoreType.DMA((4,)),
            pltpu.SemaphoreType.DMA((4,)),
        ],
        compiler_params=pltpu.CompilerParams(collective_id=0, has_side_effects=True, vmem_limit_bytes=VMEM_BYTES),
        name="gather",
    )(small, wqkv, wo, wu, wd, tok, cot)


FIRST, SECOND = 1024, 2688
SPARE_QKV, SPARE_UP = 896, 1152
DOWN_AT = 1536
SHARES = ((1, 0, 1408, 0), (1, 1408, 2688, 1), (0, 0, 512, 0), (0, 512, 1024, 1))


def pack_first(i, gw, out):
    x = gw[pl.ds(pl.multiple_of(48 * i, 16), 48), :]
    for d in range(4):
        part = x[12 * d : 12 * d + 12]
        rest = jnp.concatenate([part[4 * j : 4 * j + 4, SPARE_QKV:] for j in range(3)] + [jnp.zeros((4, 128), F32)], axis=1)
        out[4 * i + d, :, 128:] = jnp.concatenate([part[:, :SPARE_QKV], rest], axis=0).astype(BF16)


def pack_second(i, gwo, gwu, out):
    at = pl.ds(pl.multiple_of(48 * i, 16), 48)
    x = jnp.concatenate([gwo[at, :], gwu[at, :]], axis=1)
    width = gwo.shape[1]
    for d in range(4):
        part = x[12 * d : 12 * d + 12]
        rest = jnp.concatenate([part[4 * j : 4 * j + 4, DOWN_AT:] for j in range(3)] + [jnp.zeros((4, width), F32)], axis=1)
        out[4 * i + d, :, :DOWN_AT] = jnp.concatenate([part[:, :DOWN_AT], rest], axis=0).astype(BF16)


def pack_down(gwd, out):
    width, ff = gwd.shape
    for b in range(ff // 128):
        turned = gwd[:, 128 * b : 128 * b + 128].T.astype(BF16)
        for r in range(8):
            k, i = divmod(8 * b + r, 3)
            out[k, :, DOWN_AT + width * i : DOWN_AT + width * (i + 1)] = turned[16 * r : 16 * r + 16]


def pack_small(vectors, wide, out):
    lane = lax.broadcasted_iota(jnp.int32, (8, 128), 1)
    for k in range(out.shape[0]):
        blocks = []
        for src, size in ((vectors, 12), (wide, 48)):
            t, by = divmod(size * k, 128)
            block = src[:, 128 * t : 128 * t + 128]
            if by:
                block = pltpu.roll(block, 128 - by, 1)
                if by + size > 128:
                    block = jnp.where(lane < 128 - by, block, pltpu.roll(src[:, 128 * t + 128 : 128 * t + 256], 128 - by, 1))
            blocks.append(block)
        out[k, :, 0:128] = jnp.concatenate(blocks, axis=0).astype(BF16)


class Scatter:
    def __init__(self, share, parts, mine, others, first, second, third, sems):
        self.block, self.lo, self.hi, self.order = SHARES[share]
        self.share, self.parts = share, parts[self.block]
        self.sum, self.core, self.first, self.second, self.third = mine, others, first, second, third
        self.send, self.core_sem, self.first_sem, self.second_sem, self.third_sem = sems
        self.x, self.c, self.z, self.y = here()
        self.lanes = slice(self.lo, self.hi)
        self.wide = slice(0, self.hi - self.lo)

    def part(self, da, db, d, core):
        dx, dy = (db, da) if self.order == 0 else (da, db)
        slab = number(1 - self.x if dx else self.x, core, lax.rem(self.z + d, LAYERS), 1 - self.y if dy else self.y)
        return self.parts.at[slab, :, self.lanes]

    def move(self, src, dst, sem, to):
        return remote(src, dst, self.send.at[self.share], sem, to)

    def slot(self, da, db, d):
        return (da * 2 + db) * LAYERS + d

    def to_core(self, da, db, d):
        s = self.slot(da, db, d)
        to = place(self.x, 1 - self.c, self.z, self.y)
        return self.move(self.part(da, db, d, 1 - self.c), self.core.at[self.share, s, :, self.wide], self.core_sem.at[self.share, s], to)

    def to_first(self, db, d):
        s = self.slot(1, db, d)
        to = place(self.x, self.c, self.z, 1 - self.y) if self.order == 0 else place(1 - self.x, self.c, self.z, self.y)
        at = db * LAYERS + d
        return self.move(self.sum.at[self.share, s, :, self.wide], self.first.at[self.share, at, :, self.wide], self.first_sem.at[self.share, at], to)

    def to_second(self, d):
        s = self.slot(0, 1, d)
        to = place(1 - self.x, self.c, self.z, self.y) if self.order == 0 else place(self.x, self.c, self.z, 1 - self.y)
        return self.move(self.sum.at[self.share, s, :, self.wide], self.second.at[self.share, d, :, self.wide], self.second_sem.at[self.share, d], to)

    def to_third(self, d):
        s = self.slot(0, 0, d)
        to = place(self.x, self.c, lax.rem(self.z + d, LAYERS), self.y)
        return self.move(self.sum.at[self.share, s, :, self.wide], self.third.at[self.share, d - 1, :, self.wide], self.third_sem.at[self.share, d - 1], to)

    def begin(self):
        for da, db in ((1, 1), (1, 0), (0, 1), (0, 0)):
            for d in (1, 2, 3, 0):
                self.to_core(da, db, d).start()

    def total(self, da, db, d):
        s = self.slot(da, db, d)
        self.to_core(da, db, d).wait_recv()
        t = self.part(da, db, d, self.c)[...].astype(F32) + self.core[self.share, s, :, self.wide].astype(F32)
        if da == 0:
            self.to_first(db, d).wait_recv()
            t = t + self.first[self.share, db * LAYERS + d, :, self.wide].astype(F32)
            if db == 0:
                self.to_second(d).wait_recv()
                t = t + self.second[self.share, d, :, self.wide].astype(F32)
        return t

    def level(self, n):
        for da, db, d in {
            0: [(1, db, d) for db in (1, 0) for d in (1, 2, 3, 0)],
            1: [(0, 1, d) for d in (1, 2, 3, 0)],
            2: [(0, 0, d) for d in (1, 2, 3)],
        }[n]:
            self.sum[self.share, self.slot(da, db, d), :, self.wide] = self.total(da, db, d).astype(BF16)
            (self.to_first(db, d) if n == 0 else self.to_second(d) if n == 1 else self.to_third(d)).start()

    def result(self):
        t = self.total(0, 0, 0)
        for d in (1, 2, 3):
            self.to_third(d).wait_recv()
            t = t + self.third[self.share, d - 1, :, self.wide].astype(F32)
        return t

    def finish(self):
        ref = self.parts.at[pl.ds(0, 31), :, self.lanes]
        self.move(ref, ref, self.core_sem.at[self.share, 0], place(self.x, self.c, self.z, self.y)).wait_send()


def scatter_kernel(first_in, second_in, gqkv, gwo, gwu, gwd, small, mine, core, first, second, third, *sems):
    x, c, z, y = here()
    greet(
        [place(x, c, lax.rem(z + d, LAYERS), y) for d in range(1, LAYERS)]
        + [place(1 - x, c, z, y), place(x, c, z, 1 - y), place(x, 1 - c, z, y)]
    )
    shares = [Scatter(i, (first_in, second_in), mine, core, first, second, third, sems) for i in range(len(SHARES))]
    for s in shares:
        s.begin()
    for n in range(3):
        for s in shares:
            s.level(n)
    two, one = jnp.concatenate([s.result() for s in shares[:2]], axis=1), jnp.concatenate([s.result() for s in shares[2:]], axis=1)
    width = gwo.shape[1]
    gqkv[:, :SPARE_QKV] = one[:12, 128:]
    gwo[...] = two[:12, :width]
    gwu[:, :SPARE_UP] = two[:12, width:DOWN_AT]
    for j in range(3):
        gqkv[4 * j : 4 * j + 4, SPARE_QKV:] = one[12:, 128 + 256 * j : 128 + 256 * (j + 1)]
        gwu[4 * j : 4 * j + 4, SPARE_UP:] = two[12:, width * j : width * (j + 1)]
        gwd[16 * j : 16 * j + 16, :] = two[:, DOWN_AT + width * j : DOWN_AT + width * (j + 1)]
    small[...] = one[:, :128]
    for s in shares:
        s.finish()


def scatter_all(first, second, width, ff):
    n = first.shape[0]
    vmem = pl.BlockSpec(memory_space=pltpu.VMEM)
    S = jax.ShapeDtypeStruct
    own = width // n
    k = len(SHARES)
    widest = max(hi - lo for _, lo, hi, _ in SHARES)
    return pl.pallas_call(
        scatter_kernel,
        out_shape=(S((own, 3 * width), F32), S((own, width), F32), S((own, ff), F32), S((ff // n, width), F32), S((16, 128), F32)),
        in_specs=[vmem, vmem],
        out_specs=(vmem,) * 5,
        scratch_shapes=[
            pltpu.VMEM((k, 16, 16, widest), BF16),
            pltpu.VMEM((k, 16, 16, widest), BF16),
            pltpu.VMEM((k, 8, 16, widest), BF16),
            pltpu.VMEM((k, 4, 16, widest), BF16),
            pltpu.VMEM((k, 3, 16, widest), BF16),
            pltpu.SemaphoreType.DMA((k,)),
            pltpu.SemaphoreType.DMA((k, 16)),
            pltpu.SemaphoreType.DMA((k, 8)),
            pltpu.SemaphoreType.DMA((k, 4)),
            pltpu.SemaphoreType.DMA((k, 3)),
        ],
        compiler_params=pltpu.CompilerParams(collective_id=1, has_side_effects=True, vmem_limit_bytes=VMEM_BYTES),
        name="scatter",
    )(first, second)


def small_parameters(vectors, wide):
    block = jnp.stack(list(vectors), axis=0)
    block = jnp.pad(block, ((0, 0), (0, 128 - block.shape[1])))
    return jnp.concatenate([block, jnp.pad(wide[None, :], ((0, 7), (0, 128 - wide.shape[0])))], axis=0)


def per_device(
    tokens, cotangent, image_start, image_end, qkv_weight, q_bias, v_bias, out_weight, out_bias, up_weight, up_bias,
    down_weight, down_bias, first_gain, first_bias, second_gain, second_bias,
):
    width, ff = tokens.shape[1], up_weight.shape[1]
    vectors = (q_bias, v_bias, out_bias, down_bias, first_gain, first_bias, second_gain, second_bias)
    packs = lax.axis_size("dp") == COLS * CORES and lax.axis_size("fsdp") == LAYERS * ROWS_UP
    if packs:
        small = small_parameters(vectors, up_bias)
        wqkv, wo, wu, wd, vec, upb, tokh, coth = gather_all(small, qkv_weight, out_weight, up_weight, down_weight, tokens, cotangent)
    else:
        whole = lambda a: lax.all_gather(a, AXES, axis=0, tiled=True)
        wqkv, wo, wu, wd = (whole(a) for a in (qkv_weight, out_weight, up_weight, down_weight))
        vec = jnp.stack([whole(a).astype(F32) for a in vectors])
        upb = jnp.broadcast_to(whole(up_bias).astype(F32)[None, :], (8, ff))
        n = lax.axis_size(AXES)
        up, down = [(i, i + 1) for i in range(n - 1)], [(i + 1, i) for i in range(n - 1)]
        side = lambda a: jnp.concatenate([lax.ppermute(a[a.shape[0] - LEFT :], AXES, up), lax.ppermute(a[:RIGHT], AXES, down)])
        tokh, coth = side(tokens), side(cotangent)
    qkv, qkvh = project(tokens, tokh, wqkv, vec)
    layer, dhid, dqkv, gvec, gupb, *grads = middle(
        packs, image_start, image_end, qkv, qkvh, tokens, tokh, cotangent, coth, wo, wu, wd, vec, upb
    )
    dx, *grads1 = last(packs, tokens, dhid, dqkv, wqkv, vec, gvec, gupb)
    if packs:
        gqkv, gwo, gwu, gwd, sums = scatter_all(grads1[0], grads[0], width, ff)
        sums, ups = sums[:8, : q_bias.shape[0]], sums[8, : up_bias.shape[0]]
    else:
        reduced = lambda a: lax.psum_scatter(a, AXES, scatter_dimension=0, tiled=True)
        gqkv, gwo, gwu, gwd = (reduced(a) for a in (grads1[0], grads[0], grads[1], grads[2].T))
        sums, ups = reduced(grads1[1].T).T, reduced(gupb[0])
    return (
        layer, dx, gqkv, sums[0], sums[1], gwo, sums[2], gwu, ups, gwd, sums[3], sums[4], sums[5], sums[6], sums[7],
    )


def solution(mesh):
    both = P(AXES, None)
    one = P(AXES)
    in_specs = (both, both, one, one, both, one, one, both, one, both, one, both, one, one, one, one, one)
    out_specs = (both, both, both, one, one, both, one, both, one, both, one, one, one, one, one)
    return jax.shard_map(per_device, mesh=mesh, in_specs=in_specs, out_specs=out_specs, check_vma=False)
```

```python
import functools
import math

import jax
import jax.numpy as jnp
from jax import lax
from jax.experimental import pallas as pl
from jax.experimental.pallas import tpu as pltpu
from jax.sharding import PartitionSpec as P

F32 = jnp.float32
BF16 = jnp.bfloat16
HDIM = 64
EPS = 1e-06
NEG = -1e30
ROOT_HALF = 0.7071067811865476
GAUSS = 0.3989422804014327
LEFT = 112
RIGHT = 160
HALO = LEFT + RIGHT
KEYS = 224
WIN = 256
SPARE = 64
SHORTEST, LONGEST = 98, 197
AXES = ("dp", "fsdp")
VMEM_BYTES = 63 * 1024 * 1024


def dot(a, b):
    return jnp.dot(a, b, preferred_element_type=F32)


def dot_nt(a, b):
    return lax.dot_general(a, b, (((1,), (1,)), ((), ())), preferred_element_type=F32)


def dot_tn(a, b):
    return lax.dot_general(a, b, (((0,), (0,)), ((), ())), preferred_element_type=F32)


def normed(x):
    centre = x - jnp.mean(x, axis=-1, keepdims=True)
    inverse = lax.rsqrt(jnp.mean(centre * centre, axis=-1, keepdims=True) + EPS)
    return centre * inverse, inverse


def norm_back(grad, xhat, inverse, gain):
    e = grad * gain
    return inverse * (
        e - jnp.mean(e, axis=-1, keepdims=True) - xhat * jnp.mean(e * xhat, axis=-1, keepdims=True)
    )


def colsum(x):
    return jnp.sum(x, axis=0, keepdims=True)


def qkv_rows(rows, weight, gain, shift, bias, width):
    xhat, _ = normed(rows.astype(F32))
    n1 = (xhat * gain + shift).astype(BF16)
    out = dot(n1, weight) + bias
    return jnp.concatenate([out[:, :width] * (1.0 / math.sqrt(HDIM)), out[:, width:]], axis=1).astype(BF16)


def qkv_kernel(tok, tokh, weight, vec, out, outh):
    width = tok.shape[1]
    gain, shift = vec[4:5, :], vec[5:6, :]
    bias = jnp.concatenate([vec[0:1, :], jnp.zeros((1, width), F32), vec[1:2, :]], axis=1)
    out[...] = qkv_rows(tok[...], weight[...], gain, shift, bias, width)

    @pl.when(pl.program_id(0) == pl.num_programs(0) - 1)
    def _():
        outh[...] = qkv_rows(tokh[...], weight[...], gain, shift, bias, width)


def project(tok, tokh, weight, vec):
    rows, width = tok.shape
    tile = 512
    whole = lambda a: pl.BlockSpec(a.shape, lambda i: (0, 0))
    wide = weight.shape[1]
    return pl.pallas_call(
        qkv_kernel,
        grid=(rows // tile,),
        out_shape=(jax.ShapeDtypeStruct((rows, wide), BF16), jax.ShapeDtypeStruct((HALO, wide), BF16)),
        in_specs=[pl.BlockSpec((tile, width), lambda i: (i, 0))] + [whole(a) for a in (tokh, weight, vec)],
        out_specs=(pl.BlockSpec((tile, wide), lambda i: (i, 0)), pl.BlockSpec((HALO, wide), lambda i: (0, 0))),
        name="project",
    )(tok, tokh, weight, vec)


def image_bounds(i, starts, ends):
    s, e = starts[i], ends[i]
    a = pl.multiple_of((s // 16) * 16, 16)
    return s, e, a


def put(ref, a, columns, value, first_row, old):
    rows = value.shape[0]
    row = lax.broadcasted_iota(jnp.int32, (16, value.shape[1]), 0) + a
    ref[pl.ds(a, 16), columns] = jnp.where(row >= first_row, value[:16].astype(F32), old[:, columns].astype(F32)).astype(ref.dtype)
    ref[pl.ds(a + 16, rows - 16), columns] = value[16:].astype(ref.dtype)


def lane_masks(rows):
    lane = lax.broadcasted_iota(jnp.int32, (rows, 128), 1)
    low = jnp.where(lane < HDIM, 1.0, 0.0)
    return low.astype(BF16), (1.0 - low).astype(BF16)


def attention_forward(i, starts, ends, qkv, probs, att, width):
    s, e, a = image_bounds(i, starts, ends)
    row = lax.broadcasted_iota(jnp.int32, (KEYS, 1), 0) + a
    inside = (row >= s) & (row < e)
    key_bias = jnp.where(inside, 0.0, NEG)
    col = lax.broadcasted_iota(jnp.int32, (1, WIN), 1) + a
    query_on = jnp.where((col >= s) & (col < e), 1.0, 0.0)
    masks = lane_masks(KEYS)
    old_probs, old_att = probs[pl.ds(a, 16), :], att[pl.ds(a, 16), :]
    for pair in range(width // 128):
        lanes = slice(128 * pair, 128 * pair + 128)
        q = qkv[pl.ds(a, WIN), lanes]
        k = qkv[pl.ds(a, KEYS), width + 128 * pair : width + 128 * pair + 128]
        v = qkv[pl.ds(a, KEYS), 2 * width + 128 * pair : 2 * width + 128 * pair + 128]
        total = None
        for half in range(2):
            head = 2 * pair + half
            scores = dot_nt(k * masks[half], q) + key_bias
            top = jnp.max(scores, axis=0, keepdims=True)
            ex = jnp.exp(scores - top)
            p = (ex * (query_on / jnp.sum(ex, axis=0, keepdims=True))).astype(BF16)
            put(probs, a, slice(WIN * head, WIN * head + WIN), p, s, old_probs)
            part = dot_tn(p, v * masks[half])
            total = part if total is None else total + part
        put(att, a, lanes, total, s, old_att)


def attention_backward(i, starts, ends, qkv, probs, att, datt, dqkv, gvec, width, rows):
    s, e, a = image_bounds(i, starts, ends)
    scale = 1.0 / math.sqrt(HDIM)
    row = lax.broadcasted_iota(jnp.int32, (KEYS, 128), 0) + a
    inside = jnp.where((row >= s) & (row < e), 1.0, 0.0).astype(BF16)
    key_masks = [m * inside for m in lane_masks(KEYS)]
    masks = lane_masks(KEYS)
    wide_masks = lane_masks(WIN)
    query = lax.broadcasted_iota(jnp.int32, (WIN, 128), 0) + a
    own = jnp.where((query >= LEFT) & (query < LEFT + rows), 1.0, 0.0)
    group = lax.broadcasted_iota(jnp.int32, (8, width), 1) // HDIM
    heads = jnp.where(group == lax.broadcasted_iota(jnp.int32, (8, width), 0), 1.0, 0.0).astype(BF16)
    both = att[pl.ds(a, WIN), :].astype(F32) * datt[pl.ds(a, WIN), :].astype(F32)
    high = both.astype(BF16)
    old = dqkv[pl.ds(a, 16), :]
    delta = dot_nt(heads, high) + dot_nt(heads, (both - high.astype(F32)).astype(BF16))
    for pair in range(width // 128):
        lanes = slice(128 * pair, 128 * pair + 128)
        klanes = slice(width + 128 * pair, width + 128 * pair + 128)
        vlanes = slice(2 * width + 128 * pair, 2 * width + 128 * pair + 128)
        q = qkv[pl.ds(a, WIN), lanes]
        k = qkv[pl.ds(a, KEYS), klanes]
        v = qkv[pl.ds(a, KEYS), vlanes]
        do = datt[pl.ds(a, WIN), lanes]
        dq = dk = dv = None
        for half in range(2):
            head = 2 * pair + half
            p = probs[pl.ds(a, KEYS), WIN * head : WIN * head + WIN]
            dp = dot_nt(v * masks[half], do)
            ds = (p.astype(F32) * (dp - delta[head : head + 1])).astype(BF16)
            dv_part = dot(p, do * wide_masks[half])
            dk_part = dot(ds, q * wide_masks[half])
            dq_part = dot_tn(ds, k * key_masks[half])
            dv = dv_part if dv is None else dv + dv_part
            dk = dk_part if dk is None else dk + dk_part
            dq = dq_part if dq is None else dq + dq_part
        gvec[0:1, lanes] += colsum(dq * own) * scale
        put(dqkv, a, lanes, dq * scale, s, old)
        put(dqkv, a, klanes, dk, s, old)
        put(dqkv, a, vlanes, dv, s, old)


def middle_kernel(
    packs, start_in, end_in, qkv_in, qkvh_in, tok_in, tokh, cot_in, coth, wqkv, wo, wu, wd, vec, upb, out_hbm, dx_hbm, *refs
):
    first_hbm, second_hbm, first, second = (None,) * 4
    if packs:
        first_hbm, second_hbm, first, second, *refs = refs
        gsum, gupb, gwo, gwu, gwd, *refs = refs
        gw = gwu.at[:, : 3 * wo.shape[0]]
    else:
        gsum, gupb, gw, gwo, gwu, gwd, *refs = refs
    qkv, dqkv, probs, att, datt, tok, cot, out_buf, row_buf, starts, ends, sems = refs
    rows, width = tok_in.shape
    ff = wu.shape[1]
    chunk = ff
    extent = rows + HALO
    tile = out_buf.shape[1]
    early = rows // 3
    copies = [
        pltpu.make_async_copy(qkvh_in.at[pl.ds(0, LEFT)], qkv.at[pl.ds(0, LEFT)], sems.at[0]),
        pltpu.make_async_copy(qkv_in.at[pl.ds(0, early)], qkv.at[pl.ds(LEFT, early)], sems.at[1]),
    ]
    rest = [
        pltpu.make_async_copy(qkv_in.at[pl.ds(early, rows - early)], qkv.at[pl.ds(LEFT + early, rows - early)], sems.at[2]),
        pltpu.make_async_copy(qkvh_in.at[pl.ds(LEFT, RIGHT)], qkv.at[pl.ds(LEFT + rows, RIGHT)], sems.at[3]),
    ]
    later = [
        pltpu.make_async_copy(tok_in, tok, sems.at[4]),
        pltpu.make_async_copy(cot_in, cot, sems.at[5]),
    ]
    for c in copies + rest + later:
        c.start()

    shift = LEFT - lax.axis_index(AXES) * rows
    starts[0] = start_in[0] + shift
    ends[0] = end_in[0] + shift

    def walk(i, n):
        here = ends[i - 1]
        more = here < LEFT + rows
        at = jnp.minimum(here - LEFT, rows - 1)
        starts[i] = here
        ends[i] = end_in[at] + shift
        return jnp.where(more, i + 1, n)

    count = lax.fori_loop(1, starts.shape[0], walk, 1)

    spare = qkv.shape[0] - extent
    qkv[pl.ds(extent, spare), :] = jnp.zeros((spare, qkv.shape[1]), BF16)
    datt[pl.ds(extent, spare), :] = jnp.zeros((spare, width), BF16)
    probs[pl.ds(0, LEFT), :] = jnp.zeros((LEFT, probs.shape[1]), BF16)
    att[pl.ds(0, LEFT), :] = jnp.zeros((LEFT, width), BF16)
    att[pl.ds(LEFT + rows, RIGHT + spare), :] = jnp.zeros((RIGHT + spare, width), BF16)
    dqkv[pl.ds(0, LEFT), :] = jnp.zeros((LEFT, dqkv.shape[1]), BF16)
    for c in copies:
        c.wait()

    assert 3 * LONGEST + WIN <= early and rows > 5 * LONGEST

    @pl.loop(0, count)
    def _(i):
        @pl.when(i == 4)
        def _():
            for c in rest:
                c.wait()

        attention_forward(i, starts, ends, qkv, probs, att, width)

    bo, bd, g1, b1, g2, b2 = (vec[j : j + 1, :] for j in (2, 3, 4, 5, 6, 7))

    def feed(x, c, at, own):
        hid = x.astype(F32) + dot(at, wo[...]) + bo
        xhat, inverse = normed(hid)
        n2 = (xhat * g2 + b2).astype(BF16)
        down = dn2 = None
        if own:
            ct, nt = c.T, n2.T
        for f in range(0, ff, chunk):
            cols = slice(f, f + chunk)
            pre = dot(n2, wu[:, cols]) + upb[0:1, cols]
            half = 0.5 * (1.0 + lax.erf(pre * ROOT_HALF))
            slope = half + pre * jnp.exp(-0.5 * pre * pre) * GAUSS
            dpre = dot_nt(c, wd[cols, :]) * slope
            dpre_b = dpre.astype(BF16)
            part = dot_nt(dpre_b, wu[:, cols])
            dn2 = part if dn2 is None else dn2 + part
            if own:
                act = (pre * half).astype(BF16)
                part = dot(act, wd[cols, :])
                down = part if down is None else down + part
                gwd[:, cols] += dot(ct, act)
                gwu[:, cols] += dot(nt, dpre_b)
                gupb[0:1, cols] += colsum(dpre)
        dhid = c.astype(F32) + norm_back(dn2, xhat, inverse, g2)
        dhid_b = dhid.astype(BF16)
        da = dot_nt(dhid_b, wo[...]).astype(BF16)
        if own:
            gwo[...] += dot_tn(at, dhid_b)
            for j, x in ((2, dhid), (3, c.astype(F32)), (6, dn2 * xhat), (7, dn2)):
                gsum[j : j + 1, :] += colsum(x)
            return hid + down + bd, dhid, da
        return da

    gwo[...] = jnp.zeros_like(gwo)
    gwu[...] = jnp.zeros_like(gwu)
    gwd[...] = jnp.zeros_like(gwd)
    gsum[...] = jnp.zeros_like(gsum)
    gupb[...] = jnp.zeros_like(gupb)
    for c in later:
        c.wait()

    def tile_at(i):
        return pl.ds(pl.multiple_of(i * tile, tile), tile)

    def layer_write(i):
        return pltpu.make_async_copy(out_buf.at[i % 2], out_hbm.at[tile_at(i)], sems.at[6 + i % 2])

    def row_write(i, first_slot):
        slot = first_slot + i % 2
        return pltpu.make_async_copy(row_buf.at[slot], dx_hbm.at[tile_at(i)], sems.at[8 + slot])

    def row_read(i):
        return pltpu.make_async_copy(dx_hbm.at[tile_at(i)], row_buf.at[i % 2], sems.at[12 + i % 2])

    tiles = rows // tile

    @pl.loop(0, tiles)
    def _(i):
        at = pl.multiple_of(i * tile, tile)
        here = pl.ds(pl.multiple_of(LEFT + at, 16), tile)
        layer, dhid, da = feed(tok[pl.ds(at, tile), :], cot[pl.ds(at, tile), :], att[here, :], True)
        datt[here, :] = da

        @pl.when(i >= 2)
        def _():
            layer_write(i - 2).wait()
            row_write(i - 2, 0).wait()

        out_buf[i % 2] = layer.astype(BF16)
        row_buf[i % 2] = dhid
        layer_write(i).start()
        row_write(i, 0).start()

    sides = jnp.concatenate([att[pl.ds(0, LEFT), :], att[pl.ds(LEFT + rows, RIGHT), :]], axis=0)
    da = feed(tokh[...], coth[...], sides, False)
    datt[pl.ds(0, LEFT), :] = da[:LEFT]
    datt[pl.ds(LEFT + rows, RIGHT), :] = da[LEFT:]

    if packs:

        @pl.loop(0, second.shape[0] // 4)
        def _(i):
            pack_second(i, gwo, gwu, second)

        pack_down(gwd, second)
        second_sent = pltpu.make_async_copy(second, second_hbm, sems.at[14])
        second_sent.start()

    for i in (tiles - 2, tiles - 1):
        row_write(i, 0).wait()
    row_read(0).start()
    gw[...] = jnp.zeros(gw.shape, F32)

    @pl.loop(0, count)
    def _(i):
        attention_backward(i, starts, ends, qkv, probs, att, datt, dqkv, gsum, width, rows)

    @pl.loop(0, tiles)
    def _(i):
        at = pl.multiple_of(i * tile, tile)
        row_read(i).wait()

        @pl.when(i + 1 < tiles)
        def _():
            row_read(i + 1).start()

        @pl.when(i >= 2)
        def _():
            row_write(i - 2, 2).wait()

        d = dqkv[pl.ds(pl.multiple_of(LEFT + at, 16), tile), :]
        xhat, inverse = normed(tok[pl.ds(at, tile), :].astype(F32))
        n1 = (xhat * g1 + b1).astype(BF16)
        gw[...] += dot(n1.T, d)
        dn1 = dot_nt(d, wqkv[...])
        for j, x in ((1, d[:, 2 * width :].astype(F32)), (4, dn1 * xhat), (5, dn1)):
            gsum[j : j + 1, :] += colsum(x)
        row_buf[2 + i % 2] = row_buf[i % 2] + norm_back(dn1, xhat, inverse, g1)
        row_write(i, 2).start()

    if packs:

        @pl.loop(0, first.shape[0] // 4)
        def _(i):
            pack_first(i, gw, first)

        pack_small(gsum[...], gupb[...], first)
        first_sent = pltpu.make_async_copy(first, first_hbm, sems.at[15])
        first_sent.start()
        first_sent.wait()
        second_sent.wait()
    for i in (tiles - 2, tiles - 1):
        layer_write(i).wait()
        row_write(i, 2).wait()


def middle(packs, start, end, qkv, qkvh, tok, tokh, cot, coth, wqkv, wo, wu, wd, vec, upb):
    rows, width = tok.shape
    ff = wu.shape[1]
    padded = rows + HALO + SPARE
    tile = 512
    vmem = pl.BlockSpec(memory_space=pltpu.VMEM)
    smem = pl.BlockSpec(memory_space=pltpu.SMEM)
    anyw = pl.BlockSpec(memory_space=pl.ANY)
    most = rows // SHORTEST + 4
    n = lax.axis_size(AXES)
    S = jax.ShapeDtypeStruct
    sums = [((8, width), F32), ((8, ff), F32), ((width, 3 * width), F32), ((width, width), F32), ((width, ff), F32), ((width, ff), F32)]
    slabs = [((n, 16, FIRST), BF16), ((n, 16, SECOND), BF16)]
    held = slabs + [a for i, a in enumerate(sums) if i != 2] if packs else []
    return pl.pallas_call(
        functools.partial(middle_kernel, packs),
        out_shape=[S((rows, width), BF16), S((rows, width), F32)] + [S(*a) for a in (slabs if packs else sums)],
        in_specs=[smem, smem, anyw, anyw, anyw, vmem, anyw] + [vmem] * 7,
        out_specs=[anyw, anyw] + ([anyw] * 2 if packs else [vmem] * 6),
        scratch_shapes=[pltpu.VMEM(*a) for a in held]
        + [
            pltpu.VMEM((padded, 3 * width), BF16),
            pltpu.VMEM((padded, 3 * width), BF16),
            pltpu.VMEM((padded, width // HDIM * WIN), BF16),
            pltpu.VMEM((padded, width), BF16),
            pltpu.VMEM((padded, width), BF16),
            pltpu.VMEM((rows, width), BF16),
            pltpu.VMEM((rows, width), BF16),
            pltpu.VMEM((2, tile, width), BF16),
            pltpu.VMEM((4, tile, width), F32),
            pltpu.SMEM((most,), jnp.int32),
            pltpu.SMEM((most,), jnp.int32),
            pltpu.SemaphoreType.DMA((16,)),
        ],
        compiler_params=pltpu.CompilerParams(vmem_limit_bytes=VMEM_BYTES),
        name="middle",
    )(start, end, qkv, qkvh, tok, tokh, cot, coth, wqkv, wo, wu, wd, vec, upb)


COLS, ROWS_UP, LAYERS, CORES = 2, 2, 4, 2
LANES = 3584
SMALL, QKV, OUT, UP, DOWN = 0, 128, 1280, 1664, 2432
PIECES = ((0, 640, 0), (640, 1280, 1), (1280, 2432, 0), (2432, 3584, 1))
MESH = pl.DeviceIdType.MESH


def here():
    dp, fs = lax.axis_index("dp"), lax.axis_index("fsdp")
    return dp // CORES, dp % CORES, fs // ROWS_UP, fs % ROWS_UP


def place(x, c, z, y):
    return (x * CORES + c, z * ROWS_UP + y)


def number(x, c, z, y):
    return (x * CORES + c) * (LAYERS * ROWS_UP) + z * ROWS_UP + y


def greet(ids):
    barrier = pltpu.get_barrier_semaphore()
    for d in ids:
        pl.semaphore_signal(barrier, inc=1, device_id=d, device_id_type=MESH)
    pl.semaphore_wait(barrier, len(ids))


def remote(src, dst, send, recv, to):
    return pltpu.make_async_remote_copy(src_ref=src, dst_ref=dst, send_sem=send, recv_sem=recv, device_id=to, device_id_type=MESH)


def along(step):
    dp, fs = lax.axis_size("dp"), lax.axis_size("fsdp")
    at = lax.rem(lax.axis_index("dp") * fs + lax.axis_index("fsdp") + step + dp * fs, dp * fs)
    return (at // fs, lax.rem(at, fs))


class Gather:
    def __init__(self, slabs, send, recv):
        self.slabs, self.send, self.recv = slabs, send, recv
        self.x, self.c, self.z, self.y = here()

    def copy(self, piece, slab, to):
        lo, hi, _ = PIECES[piece]
        ref = self.slabs.at[slab, :, lo:hi]
        return remote(ref, ref, self.send.at[piece], self.recv.at[piece, slab], to)

    def give(self, piece, slab, axes):
        x, c, z, y = self.x, self.c, self.z, self.y
        for axis in axes:
            if axis == "z":
                for d in range(1, LAYERS):
                    self.copy(piece, slab, place(x, c, lax.rem(z + d, LAYERS), y)).start()
            else:
                to = {"x": place(1 - x, c, z, y), "y": place(x, c, z, 1 - y), "c": place(x, 1 - c, z, y)}[axis]
                self.copy(piece, slab, to).start()

    def own(self, piece):
        self.give(piece, number(self.x, self.c, self.z, self.y), "zxyc")

    def take(self, piece, slab):
        self.copy(piece, slab, place(self.x, self.c, self.z, self.y)).wait_recv()

    def stage(self, piece, level):
        x, c, z, y = self.x, self.c, self.z, self.y
        order = PIECES[piece][2]
        second, third = ("x", "y") if order == 0 else ("y", "x")
        if level == 0:
            group = [(x, lax.rem(z + d, LAYERS), y) for d in range(1, LAYERS)]
            passed = second + third + "c"
        elif level == 1:
            group = [(1 - x, lax.rem(z + d, LAYERS), y) if order == 0 else (x, lax.rem(z + d, LAYERS), 1 - y) for d in range(LAYERS)]
            passed = third + "c"
        else:
            if order == 0:
                group = [(x if s == 0 else 1 - x, lax.rem(z + d, LAYERS), 1 - y) for s in range(2) for d in range(LAYERS)]
            else:
                group = [(1 - x, lax.rem(z + d, LAYERS), y if s == 0 else 1 - y) for s in range(2) for d in range(LAYERS)]
            passed = "c"
        for gx, gz, gy in group:
            slab = number(gx, c, gz, gy)
            self.take(piece, slab)
            self.give(piece, slab, passed)

    def siblings(self, piece):
        x, c, z, y = self.x, self.c, self.z, self.y
        for dx in range(COLS):
            for dy in range(ROWS_UP):
                for d in range(LAYERS):
                    self.take(piece, number(x if dx == 0 else 1 - x, 1 - c, lax.rem(z + d, LAYERS), y if dy == 0 else 1 - y))

    def finish(self, piece):
        lo, hi, _ = PIECES[piece]
        ref = self.slabs.at[pl.ds(0, 31), :, lo:hi]
        remote(ref, ref, self.send.at[piece], self.recv.at[piece, 0], place(self.x, self.c, self.z, self.y)).wait_send()


def gather_kernel(
    small, wqkv_in, wo_in, wu_in, wd_in, tok, cot,
    wqkv, wo, wu, wd, vec, upb, tokh, coth,
    slabs, send, recv, side_send, side_recv,
):
    x, c, z, y = here()
    me = number(x, c, z, y)
    rows, width = tok.shape
    n = slabs.shape[0]
    own = slabs.at[me]
    own[:, SMALL:QKV] = small[...]
    split = 768
    up = wu_in[...].astype(F32)
    top = jnp.concatenate([wqkv_in[...].astype(F32), wo_in[...].astype(F32), up[:, :split]], axis=1)
    rest = jnp.concatenate([up[4 * i : 4 * i + 4, split:] for i in range(3)], axis=1)
    own[:, QKV:DOWN] = jnp.concatenate([top, rest], axis=0).astype(BF16)
    for i in range(3):
        own[:, DOWN + width * i : DOWN + width * (i + 1)] = wd_in[16 * i : 16 * i + 16, :]

    greet(
        [place(x, c, lax.rem(z + d, LAYERS), y) for d in range(1, LAYERS)]
        + [place(1 - x, c, z, y), place(x, c, z, 1 - y), place(x, 1 - c, z, y), along(1), along(-1)]
    )
    g = Gather(slabs, send, recv)
    for p in (0, 1):
        g.own(p)
    sides = []
    for j, (src, dst) in enumerate(((tok, tokh), (cot, coth))):
        sides.append(remote(src.at[pl.ds(rows - LEFT, LEFT)], dst.at[pl.ds(0, LEFT)], side_send.at[2 * j], side_recv.at[2 * j], along(1)))
        sides.append(remote(src.at[pl.ds(0, RIGHT)], dst.at[pl.ds(LEFT, RIGHT)], side_send.at[2 * j + 1], side_recv.at[2 * j + 1], along(-1)))
    for p in (0, 1):
        g.stage(p, 0)
    for p in (2, 3):
        g.own(p)
    for s in sides:
        s.start()
    for level in (1, 2):
        for p in (0, 1):
            g.stage(p, level)
    for level in (0, 1, 2):
        for p in (2, 3):
            g.stage(p, level)
    for p in range(4):
        g.siblings(p)
    for s in sides:
        s.wait()
    for p in range(4):
        g.finish(p)

    @pl.loop(0, n // 4)
    def _(i):
        at = pl.ds(pl.multiple_of(48 * i, 16), 48)
        parts = [slabs[4 * i + d, :, QKV:DOWN].astype(F32) for d in range(4)]
        full = jnp.concatenate([p[:12] for p in parts], axis=0).astype(BF16)
        wqkv[at, :] = full[:, : OUT - QKV]
        wo[at, :] = full[:, OUT - QKV : UP - QKV]
        wu[at, :split] = full[:, UP - QKV :]
        wu[at, split:] = jnp.concatenate([p[12:, split * j : split * (j + 1)] for p in parts for j in range(3)], axis=0).astype(BF16)
        for d in range(4):
            for j in range(3):
                wd[pl.ds(pl.multiple_of(48 * (4 * i + d) + 16 * j, 16), 16), :] = slabs[4 * i + d, :, DOWN + width * j : DOWN + width * (j + 1)]

    lane = lax.broadcasted_iota(jnp.int32, (8, 128), 1)
    lines = [jnp.zeros((8, 128), F32) for _ in range(width // 128)]
    ups = [jnp.zeros((8, 128), F32) for _ in range(upb.shape[1] // 128)]
    for k in range(n):
        s = slabs[k, :, SMALL:QKV].astype(F32)
        for tiles, block, size in ((lines, s[:8], 12), (ups, s[8:], 48)):
            t, by = divmod(size * k, 128)
            moved = pltpu.roll(block, by, 1) if by else block
            if by + size <= 128:
                tiles[t] = tiles[t] + moved
            else:
                tiles[t] = tiles[t] + jnp.where(lane >= by, moved, 0.0)
                tiles[t + 1] = tiles[t + 1] + jnp.where(lane < by, moved, 0.0)
    vec[...] = jnp.concatenate(lines, axis=1)
    upb[...] = jnp.concatenate(ups, axis=1)


def gather_all(small, wqkv, wo, wu, wd, tok, cot):
    n = lax.axis_size(AXES)
    rows, width = tok.shape
    vmem = pl.BlockSpec(memory_space=pltpu.VMEM)
    anyw = pl.BlockSpec(memory_space=pl.ANY)
    S = jax.ShapeDtypeStruct
    return pl.pallas_call(
        gather_kernel,
        out_shape=(
            S((width, wqkv.shape[1]), BF16), S((width, width), BF16), S((width, wu.shape[1]), BF16), S((wd.shape[0] * n, width), BF16),
            S((8, width), F32), S((8, wu.shape[1]), F32), S((HALO, width), BF16), S((HALO, width), BF16),
        ),
        in_specs=[vmem] * 5 + [anyw] * 2,
        out_specs=(vmem,) * 6 + (anyw,) * 2,
        scratch_shapes=[
            pltpu.VMEM((n, 16, LANES), BF16),
            pltpu.SemaphoreType.DMA((4,)),
            pltpu.SemaphoreType.DMA((4, n)),
            pltpu.SemaphoreType.DMA((4,)),
            pltpu.SemaphoreType.DMA((4,)),
        ],
        compiler_params=pltpu.CompilerParams(collective_id=0, has_side_effects=True, vmem_limit_bytes=VMEM_BYTES),
        name="gather",
    )(small, wqkv, wo, wu, wd, tok, cot)


FIRST, SECOND = 1024, 2688
SPARE_QKV, SPARE_UP = 896, 1152
DOWN_AT = 1536
SHARES = ((1, 0, 1408, 0), (1, 1408, 2688, 1), (0, 0, 512, 0), (0, 512, 1024, 1))


def pack_first(i, gw, out):
    x = gw[pl.ds(pl.multiple_of(48 * i, 16), 48), :]
    for d in range(4):
        part = x[12 * d : 12 * d + 12]
        rest = jnp.concatenate([part[4 * j : 4 * j + 4, SPARE_QKV:] for j in range(3)] + [jnp.zeros((4, 128), F32)], axis=1)
        out[4 * i + d, :, 128:] = jnp.concatenate([part[:, :SPARE_QKV], rest], axis=0).astype(BF16)


def pack_second(i, gwo, gwu, out):
    at = pl.ds(pl.multiple_of(48 * i, 16), 48)
    x = jnp.concatenate([gwo[at, :], gwu[at, :]], axis=1)
    width = gwo.shape[1]
    for d in range(4):
        part = x[12 * d : 12 * d + 12]
        rest = jnp.concatenate([part[4 * j : 4 * j + 4, DOWN_AT:] for j in range(3)] + [jnp.zeros((4, width), F32)], axis=1)
        out[4 * i + d, :, :DOWN_AT] = jnp.concatenate([part[:, :DOWN_AT], rest], axis=0).astype(BF16)


def pack_down(gwd, out):
    width, ff = gwd.shape
    for b in range(ff // 128):
        turned = gwd[:, 128 * b : 128 * b + 128].T.astype(BF16)
        for r in range(8):
            k, i = divmod(8 * b + r, 3)
            out[k, :, DOWN_AT + width * i : DOWN_AT + width * (i + 1)] = turned[16 * r : 16 * r + 16]


def pack_small(vectors, wide, out):
    lane = lax.broadcasted_iota(jnp.int32, (8, 128), 1)
    for k in range(out.shape[0]):
        blocks = []
        for src, size in ((vectors, 12), (wide, 48)):
            t, by = divmod(size * k, 128)
            block = src[:, 128 * t : 128 * t + 128]
            if by:
                block = pltpu.roll(block, 128 - by, 1)
                if by + size > 128:
                    block = jnp.where(lane < 128 - by, block, pltpu.roll(src[:, 128 * t + 128 : 128 * t + 256], 128 - by, 1))
            blocks.append(block)
        out[k, :, 0:128] = jnp.concatenate(blocks, axis=0).astype(BF16)


class Scatter:
    def __init__(self, share, parts, mine, others, first, second, third, sems):
        self.block, self.lo, self.hi, self.order = SHARES[share]
        self.share, self.parts = share, parts[self.block]
        self.sum, self.core, self.first, self.second, self.third = mine, others, first, second, third
        self.send, self.core_sem, self.first_sem, self.second_sem, self.third_sem = sems
        self.x, self.c, self.z, self.y = here()
        self.lanes = slice(self.lo, self.hi)
        self.wide = slice(0, self.hi - self.lo)

    def part(self, da, db, d, core):
        dx, dy = (db, da) if self.order == 0 else (da, db)
        slab = number(1 - self.x if dx else self.x, core, lax.rem(self.z + d, LAYERS), 1 - self.y if dy else self.y)
        return self.parts.at[slab, :, self.lanes]

    def move(self, src, dst, sem, to):
        return remote(src, dst, self.send.at[self.share], sem, to)

    def slot(self, da, db, d):
        return (da * 2 + db) * LAYERS + d

    def to_core(self, da, db, d):
        s = self.slot(da, db, d)
        to = place(self.x, 1 - self.c, self.z, self.y)
        return self.move(self.part(da, db, d, 1 - self.c), self.core.at[self.share, s, :, self.wide], self.core_sem.at[self.share, s], to)

    def to_first(self, db, d):
        s = self.slot(1, db, d)
        to = place(self.x, self.c, self.z, 1 - self.y) if self.order == 0 else place(1 - self.x, self.c, self.z, self.y)
        at = db * LAYERS + d
        return self.move(self.sum.at[self.share, s, :, self.wide], self.first.at[self.share, at, :, self.wide], self.first_sem.at[self.share, at], to)

    def to_second(self, d):
        s = self.slot(0, 1, d)
        to = place(1 - self.x, self.c, self.z, self.y) if self.order == 0 else place(self.x, self.c, self.z, 1 - self.y)
        return self.move(self.sum.at[self.share, s, :, self.wide], self.second.at[self.share, d, :, self.wide], self.second_sem.at[self.share, d], to)

    def to_third(self, d):
        s = self.slot(0, 0, d)
        to = place(self.x, self.c, lax.rem(self.z + d, LAYERS), self.y)
        return self.move(self.sum.at[self.share, s, :, self.wide], self.third.at[self.share, d - 1, :, self.wide], self.third_sem.at[self.share, d - 1], to)

    def begin(self):
        for da, db in ((1, 1), (1, 0), (0, 1), (0, 0)):
            for d in (1, 2, 3, 0):
                self.to_core(da, db, d).start()

    def total(self, da, db, d):
        s = self.slot(da, db, d)
        self.to_core(da, db, d).wait_recv()
        t = self.part(da, db, d, self.c)[...].astype(F32) + self.core[self.share, s, :, self.wide].astype(F32)
        if da == 0:
            self.to_first(db, d).wait_recv()
            t = t + self.first[self.share, db * LAYERS + d, :, self.wide].astype(F32)
            if db == 0:
                self.to_second(d).wait_recv()
                t = t + self.second[self.share, d, :, self.wide].astype(F32)
        return t

    def level(self, n):
        for da, db, d in {
            0: [(1, db, d) for db in (1, 0) for d in (1, 2, 3, 0)],
            1: [(0, 1, d) for d in (1, 2, 3, 0)],
            2: [(0, 0, d) for d in (1, 2, 3)],
        }[n]:
            self.sum[self.share, self.slot(da, db, d), :, self.wide] = self.total(da, db, d).astype(BF16)
            (self.to_first(db, d) if n == 0 else self.to_second(d) if n == 1 else self.to_third(d)).start()

    def result(self):
        t = self.total(0, 0, 0)
        for d in (1, 2, 3):
            self.to_third(d).wait_recv()
            t = t + self.third[self.share, d - 1, :, self.wide].astype(F32)
        return t

    def finish(self):
        ref = self.parts.at[pl.ds(0, 31), :, self.lanes]
        self.move(ref, ref, self.core_sem.at[self.share, 0], place(self.x, self.c, self.z, self.y)).wait_send()


def scatter_kernel(first_in, second_in, one, two, mine, core, first, second, third, *sems):
    x, c, z, y = here()
    greet(
        [place(x, c, lax.rem(z + d, LAYERS), y) for d in range(1, LAYERS)]
        + [place(1 - x, c, z, y), place(x, c, z, 1 - y), place(x, 1 - c, z, y)]
    )
    shares = [Scatter(i, (first_in, second_in), mine, core, first, second, third, sems) for i in range(len(SHARES))]
    for s in shares:
        s.begin()
    for n in range(3):
        for s in shares:
            s.level(n)
    for s in shares:
        (two if s.block else one)[:, s.lanes] = s.result()
    for s in shares:
        s.finish()


def finish_kernel(one, two, gqkv, gwo, gwu, gwd, ups, *smalls):
    width, own = gwo.shape[1], gwo.shape[0]
    gqkv[:, :SPARE_QKV] = one[:own, 128:]
    gwo[...] = two[:own, :width]
    gwu[:, :SPARE_UP] = two[:own, width:DOWN_AT]
    for j in range(3):
        gqkv[4 * j : 4 * j + 4, SPARE_QKV:] = one[own:, 128 + 256 * j : 128 + 256 * (j + 1)]
        gwu[4 * j : 4 * j + 4, SPARE_UP:] = two[own:, width * j : width * (j + 1)]
        gwd[16 * j : 16 * j + 16, :] = two[:, DOWN_AT + width * j : DOWN_AT + width * (j + 1)]
    ups[...] = one[8, : ups.shape[0]]
    for j, ref in enumerate(smalls):
        ref[...] = one[j, :own]


def finish(one, two, width, ff):
    n = lax.axis_size(AXES)
    own = width // n
    S = jax.ShapeDtypeStruct
    shapes = [(own, 3 * width), (own, width), (own, ff), (ff // n, width), (ff // n,)] + [(own,)] * 8
    return pl.pallas_call(finish_kernel, out_shape=[S(a, F32) for a in shapes], name="finish")(one, two)


def scatter_all(first, second):
    vmem = pl.BlockSpec(memory_space=pltpu.VMEM)
    S = jax.ShapeDtypeStruct
    k = len(SHARES)
    widest = max(hi - lo for _, lo, hi, _ in SHARES)
    return pl.pallas_call(
        scatter_kernel,
        out_shape=(S((16, FIRST), F32), S((16, SECOND), F32)),
        in_specs=[vmem, vmem],
        out_specs=(vmem,) * 2,
        scratch_shapes=[
            pltpu.VMEM((k, 16, 16, widest), BF16),
            pltpu.VMEM((k, 16, 16, widest), BF16),
            pltpu.VMEM((k, 8, 16, widest), BF16),
            pltpu.VMEM((k, 4, 16, widest), BF16),
            pltpu.VMEM((k, 3, 16, widest), BF16),
            pltpu.SemaphoreType.DMA((k,)),
            pltpu.SemaphoreType.DMA((k, 16)),
            pltpu.SemaphoreType.DMA((k, 8)),
            pltpu.SemaphoreType.DMA((k, 4)),
            pltpu.SemaphoreType.DMA((k, 3)),
        ],
        compiler_params=pltpu.CompilerParams(collective_id=1, has_side_effects=True, vmem_limit_bytes=VMEM_BYTES),
        name="scatter",
    )(first, second)


def small_parameters(vectors, wide):
    block = jnp.stack(list(vectors), axis=0)
    block = jnp.pad(block, ((0, 0), (0, 128 - block.shape[1])))
    return jnp.concatenate([block, jnp.pad(wide[None, :], ((0, 7), (0, 128 - wide.shape[0])))], axis=0)


def per_device(
    tokens, cotangent, image_start, image_end, qkv_weight, q_bias, v_bias, out_weight, out_bias, up_weight, up_bias,
    down_weight, down_bias, first_gain, first_bias, second_gain, second_bias,
):
    width, ff = tokens.shape[1], up_weight.shape[1]
    vectors = (q_bias, v_bias, out_bias, down_bias, first_gain, first_bias, second_gain, second_bias)
    packs = lax.axis_size("dp") == COLS * CORES and lax.axis_size("fsdp") == LAYERS * ROWS_UP
    if packs:
        small = small_parameters(vectors, up_bias)
        wqkv, wo, wu, wd, vec, upb, tokh, coth = gather_all(small, qkv_weight, out_weight, up_weight, down_weight, tokens, cotangent)
    else:
        whole = lambda a: lax.all_gather(a, AXES, axis=0, tiled=True)
        wqkv, wo, wu, wd = (whole(a) for a in (qkv_weight, out_weight, up_weight, down_weight))
        vec = jnp.stack([whole(a).astype(F32) for a in vectors])
        upb = jnp.broadcast_to(whole(up_bias).astype(F32)[None, :], (8, ff))
        n = lax.axis_size(AXES)
        up, down = [(i, i + 1) for i in range(n - 1)], [(i + 1, i) for i in range(n - 1)]
        side = lambda a: jnp.concatenate([lax.ppermute(a[a.shape[0] - LEFT :], AXES, up), lax.ppermute(a[:RIGHT], AXES, down)])
        tokh, coth = side(tokens), side(cotangent)
    qkv, qkvh = project(tokens, tokh, wqkv, vec)
    layer, dx, *grads = middle(
        packs, image_start, image_end, qkv, qkvh, tokens, tokh, cotangent, coth, wqkv, wo, wu, wd, vec, upb
    )
    if packs:
        gqkv, gwo, gwu, gwd, ups, *sums = finish(*scatter_all(*grads), width, ff)
    else:
        reduced = lambda a: lax.psum_scatter(a, AXES, scatter_dimension=0, tiled=True)
        sums, ups = reduced(grads[0].T).T, reduced(grads[1][0])
        gqkv, gwo, gwu, gwd = (reduced(a) for a in (grads[2], grads[3], grads[4], grads[5].T))
    return (
        layer, dx, gqkv, sums[0], sums[1], gwo, sums[2], gwu, ups, gwd, sums[3], sums[4], sums[5], sums[6], sums[7],
    )


def solution(mesh):
    both = P(AXES, None)
    one = P(AXES)
    in_specs = (both, both, one, one, both, one, one, both, one, both, one, both, one, one, one, one, one)
    out_specs = (both, both, both, one, one, both, one, both, one, both, one, one, one, one, one)
    return jax.shard_map(per_device, mesh=mesh, in_specs=in_specs, out_specs=out_specs, check_vma=False)
```

```python
import functools
import math

import jax
import jax.numpy as jnp
from jax import lax
from jax.experimental import pallas as pl
from jax.experimental.pallas import tpu as pltpu
from jax.sharding import PartitionSpec as P

F32 = jnp.float32
BF16 = jnp.bfloat16
HDIM = 64
EPS = 1e-06
NEG = -1e30
ROOT_HALF = 0.7071067811865476
GAUSS = 0.3989422804014327
LEFT = 112
RIGHT = 160
HALO = LEFT + RIGHT
KEYS = 224
WIN = 256
SPARE = 64
SHORTEST, LONGEST = 98, 197
AXES = ("dp", "fsdp")
VMEM_BYTES = 63 * 1024 * 1024


def dot(a, b):
    return jnp.dot(a, b, preferred_element_type=F32)


def dot_nt(a, b):
    return lax.dot_general(a, b, (((1,), (1,)), ((), ())), preferred_element_type=F32)


def dot_tn(a, b):
    return lax.dot_general(a, b, (((0,), (0,)), ((), ())), preferred_element_type=F32)


def normed(x):
    centre = x - jnp.mean(x, axis=-1, keepdims=True)
    inverse = lax.rsqrt(jnp.mean(centre * centre, axis=-1, keepdims=True) + EPS)
    return centre * inverse, inverse


def norm_back(grad, xhat, inverse, gain):
    e = grad * gain
    return inverse * (
        e - jnp.mean(e, axis=-1, keepdims=True) - xhat * jnp.mean(e * xhat, axis=-1, keepdims=True)
    )


def colsum(x):
    return jnp.sum(x, axis=0, keepdims=True)


def qkv_rows(rows, weight, gain, shift, bias, width):
    xhat, _ = normed(rows.astype(F32))
    n1 = (xhat * gain + shift).astype(BF16)
    out = dot(n1, weight) + bias
    return jnp.concatenate([out[:, :width] * (1.0 / math.sqrt(HDIM)), out[:, width:]], axis=1).astype(BF16)


def qkv_kernel(tok, tokh, weight, vec, out, outh):
    width = tok.shape[1]
    gain, shift = vec[4:5, :], vec[5:6, :]
    bias = jnp.concatenate([vec[0:1, :], jnp.zeros((1, width), F32), vec[1:2, :]], axis=1)
    out[...] = qkv_rows(tok[...], weight[...], gain, shift, bias, width)

    @pl.when(pl.program_id(0) == pl.num_programs(0) - 1)
    def _():
        outh[...] = qkv_rows(tokh[...], weight[...], gain, shift, bias, width)


def project(tok, tokh, weight, vec):
    rows, width = tok.shape
    tile = 512
    whole = lambda a: pl.BlockSpec(a.shape, lambda i: (0, 0))
    wide = weight.shape[1]
    return pl.pallas_call(
        qkv_kernel,
        grid=(rows // tile,),
        out_shape=(jax.ShapeDtypeStruct((rows, wide), BF16), jax.ShapeDtypeStruct((HALO, wide), BF16)),
        in_specs=[pl.BlockSpec((tile, width), lambda i: (i, 0))] + [whole(a) for a in (tokh, weight, vec)],
        out_specs=(pl.BlockSpec((tile, wide), lambda i: (i, 0)), pl.BlockSpec((HALO, wide), lambda i: (0, 0))),
        name="project",
    )(tok, tokh, weight, vec)


def image_bounds(i, starts, ends):
    s, e = starts[i], ends[i]
    a = pl.multiple_of((s // 16) * 16, 16)
    return s, e, a


def put(ref, a, columns, value, first_row, old):
    rows = value.shape[0]
    row = lax.broadcasted_iota(jnp.int32, (16, value.shape[1]), 0) + a
    ref[pl.ds(a, 16), columns] = jnp.where(row >= first_row, value[:16].astype(F32), old[:, columns].astype(F32)).astype(ref.dtype)
    ref[pl.ds(a + 16, rows - 16), columns] = value[16:].astype(ref.dtype)


def lane_masks(rows):
    lane = lax.broadcasted_iota(jnp.int32, (rows, 128), 1)
    low = jnp.where(lane < HDIM, 1.0, 0.0)
    return low.astype(BF16), (1.0 - low).astype(BF16)


def attention_forward(i, starts, ends, qkv, probs, att, width):
    s, e, a = image_bounds(i, starts, ends)
    row = lax.broadcasted_iota(jnp.int32, (KEYS, 1), 0) + a
    inside = (row >= s) & (row < e)
    key_bias = jnp.where(inside, 0.0, NEG)
    col = lax.broadcasted_iota(jnp.int32, (1, WIN), 1) + a
    query_on = jnp.where((col >= s) & (col < e), 1.0, 0.0)
    masks = lane_masks(KEYS)
    old_probs, old_att = probs[pl.ds(a, 16), :], att[pl.ds(a, 16), :]
    for pair in range(width // 128):
        lanes = slice(128 * pair, 128 * pair + 128)
        q = qkv[pl.ds(a, WIN), lanes]
        k = qkv[pl.ds(a, KEYS), width + 128 * pair : width + 128 * pair + 128]
        v = qkv[pl.ds(a, KEYS), 2 * width + 128 * pair : 2 * width + 128 * pair + 128]
        total = None
        for half in range(2):
            head = 2 * pair + half
            scores = dot_nt(k * masks[half], q) + key_bias
            top = jnp.max(scores, axis=0, keepdims=True)
            ex = jnp.exp(scores - top)
            p = (ex * (query_on / jnp.sum(ex, axis=0, keepdims=True))).astype(BF16)
            put(probs, a, slice(WIN * head, WIN * head + WIN), p, s, old_probs)
            part = dot_tn(p, v * masks[half])
            total = part if total is None else total + part
        put(att, a, lanes, total, s, old_att)


def attention_backward(i, starts, ends, qkv, probs, att, datt, dqkv, gvec, width, rows):
    s, e, a = image_bounds(i, starts, ends)
    scale = 1.0 / math.sqrt(HDIM)
    row = lax.broadcasted_iota(jnp.int32, (KEYS, 128), 0) + a
    inside = jnp.where((row >= s) & (row < e), 1.0, 0.0).astype(BF16)
    key_masks = [m * inside for m in lane_masks(KEYS)]
    masks = lane_masks(KEYS)
    wide_masks = lane_masks(WIN)
    query = lax.broadcasted_iota(jnp.int32, (WIN, 128), 0) + a
    own = jnp.where((query >= LEFT) & (query < LEFT + rows), 1.0, 0.0)
    group = lax.broadcasted_iota(jnp.int32, (8, width), 1) // HDIM
    heads = jnp.where(group == lax.broadcasted_iota(jnp.int32, (8, width), 0), 1.0, 0.0).astype(BF16)
    both = att[pl.ds(a, WIN), :].astype(F32) * datt[pl.ds(a, WIN), :].astype(F32)
    high = both.astype(BF16)
    old = dqkv[pl.ds(a, 16), :]
    delta = dot_nt(heads, high) + dot_nt(heads, (both - high.astype(F32)).astype(BF16))
    for pair in range(width // 128):
        lanes = slice(128 * pair, 128 * pair + 128)
        klanes = slice(width + 128 * pair, width + 128 * pair + 128)
        vlanes = slice(2 * width + 128 * pair, 2 * width + 128 * pair + 128)
        q = qkv[pl.ds(a, WIN), lanes]
        k = qkv[pl.ds(a, KEYS), klanes]
        v = qkv[pl.ds(a, KEYS), vlanes]
        do = datt[pl.ds(a, WIN), lanes]
        dq = dk = dv = None
        for half in range(2):
            head = 2 * pair + half
            p = probs[pl.ds(a, KEYS), WIN * head : WIN * head + WIN]
            dp = dot_nt(v * masks[half], do)
            ds = (p.astype(F32) * (dp - delta[head : head + 1])).astype(BF16)
            dv_part = dot(p, do * wide_masks[half])
            dk_part = dot(ds, q * wide_masks[half])
            dq_part = dot_tn(ds, k * key_masks[half])
            dv = dv_part if dv is None else dv + dv_part
            dk = dk_part if dk is None else dk + dk_part
            dq = dq_part if dq is None else dq + dq_part
        gvec[0:1, lanes] += colsum(dq * own) * scale
        put(dqkv, a, lanes, dq * scale, s, old)
        put(dqkv, a, klanes, dk, s, old)
        put(dqkv, a, vlanes, dv, s, old)


def middle_kernel(
    packs, start_in, end_in, qkv_in, qkvh_in, tok_in, tokh, cot_in, coth, wqkv, wo, wu, wd, vec, upb, out_hbm, dx_hbm, *refs
):
    first_hbm, second_hbm, first, second = (None,) * 4
    if packs:
        first_hbm, second_hbm, first, second, *refs = refs
        gsum, gupb, gwo, gwu, gwd, *refs = refs
        gw = gwu.at[:, : 3 * wo.shape[0]]
    else:
        gsum, gupb, gw, gwo, gwu, gwd, *refs = refs
    qkv, dqkv, probs, att, datt, tok, cot, out_buf, row_buf, starts, ends, sems = refs
    rows, width = tok_in.shape
    ff = wu.shape[1]
    chunk = ff
    extent = rows + HALO
    tile = out_buf.shape[1]
    early = rows // 3
    copies = [
        pltpu.make_async_copy(qkvh_in.at[pl.ds(0, LEFT)], qkv.at[pl.ds(0, LEFT)], sems.at[0]),
        pltpu.make_async_copy(qkv_in.at[pl.ds(0, early)], qkv.at[pl.ds(LEFT, early)], sems.at[1]),
    ]
    rest = [
        pltpu.make_async_copy(qkv_in.at[pl.ds(early, rows - early)], qkv.at[pl.ds(LEFT + early, rows - early)], sems.at[2]),
        pltpu.make_async_copy(qkvh_in.at[pl.ds(LEFT, RIGHT)], qkv.at[pl.ds(LEFT + rows, RIGHT)], sems.at[3]),
    ]
    later = [
        pltpu.make_async_copy(tok_in, tok, sems.at[4]),
        pltpu.make_async_copy(cot_in, cot, sems.at[5]),
    ]
    for c in copies + rest + later:
        c.start()

    shift = LEFT - lax.axis_index(AXES) * rows
    starts[0] = start_in[0] + shift
    ends[0] = end_in[0] + shift

    def walk(i, n):
        here = ends[i - 1]
        more = here < LEFT + rows
        at = jnp.minimum(here - LEFT, rows - 1)
        starts[i] = here
        ends[i] = end_in[at] + shift
        return jnp.where(more, i + 1, n)

    count = lax.fori_loop(1, starts.shape[0], walk, 1)

    spare = qkv.shape[0] - extent
    qkv[pl.ds(extent, spare), :] = jnp.zeros((spare, qkv.shape[1]), BF16)
    datt[pl.ds(extent, spare), :] = jnp.zeros((spare, width), BF16)
    probs[pl.ds(0, LEFT), :] = jnp.zeros((LEFT, probs.shape[1]), BF16)
    att[pl.ds(0, LEFT), :] = jnp.zeros((LEFT, width), BF16)
    att[pl.ds(LEFT + rows, RIGHT + spare), :] = jnp.zeros((RIGHT + spare, width), BF16)
    dqkv[pl.ds(0, LEFT), :] = jnp.zeros((LEFT, dqkv.shape[1]), BF16)
    for c in copies:
        c.wait()

    assert 3 * LONGEST + WIN <= early and rows > 5 * LONGEST

    @pl.loop(0, count)
    def _(i):
        @pl.when(i == 4)
        def _():
            for c in rest:
                c.wait()

        attention_forward(i, starts, ends, qkv, probs, att, width)

    bo, bd, g1, b1, g2, b2 = (vec[j : j + 1, :] for j in (2, 3, 4, 5, 6, 7))

    def feed(x, c, at, own):
        hid = x.astype(F32) + dot(at, wo[...]) + bo
        xhat, inverse = normed(hid)
        n2 = (xhat * g2 + b2).astype(BF16)
        down = dn2 = None
        if own:
            ct, nt = c.T, n2.T
        for f in range(0, ff, chunk):
            cols = slice(f, f + chunk)
            pre = dot(n2, wu[:, cols]) + upb[0:1, cols]
            half = 0.5 * (1.0 + lax.erf(pre * ROOT_HALF))
            slope = half + pre * jnp.exp(-0.5 * pre * pre) * GAUSS
            dpre = dot_nt(c, wd[cols, :]) * slope
            dpre_b = dpre.astype(BF16)
            part = dot_nt(dpre_b, wu[:, cols])
            dn2 = part if dn2 is None else dn2 + part
            if own:
                act = (pre * half).astype(BF16)
                part = dot(act, wd[cols, :])
                down = part if down is None else down + part
                gwd[:, cols] += dot(ct, act)
                gwu[:, cols] += dot(nt, dpre_b)
                gupb[0:1, cols] += colsum(dpre)
        dhid = c.astype(F32) + norm_back(dn2, xhat, inverse, g2)
        dhid_b = dhid.astype(BF16)
        da = dot_nt(dhid_b, wo[...]).astype(BF16)
        if own:
            gwo[...] += dot_tn(at, dhid_b)
            for j, x in ((2, dhid), (3, c.astype(F32)), (6, dn2 * xhat), (7, dn2)):
                gsum[j : j + 1, :] += colsum(x)
            return hid + down + bd, dhid, da
        return da

    gwo[...] = jnp.zeros_like(gwo)
    gwu[...] = jnp.zeros_like(gwu)
    gwd[...] = jnp.zeros_like(gwd)
    gsum[...] = jnp.zeros_like(gsum)
    gupb[...] = jnp.zeros_like(gupb)
    for c in later:
        c.wait()

    def tile_at(i):
        return pl.ds(pl.multiple_of(i * tile, tile), tile)

    def layer_write(i):
        return pltpu.make_async_copy(out_buf.at[i % 2], out_hbm.at[tile_at(i)], sems.at[6 + i % 2])

    def row_write(i, first_slot):
        slot = first_slot + i % 2
        return pltpu.make_async_copy(row_buf.at[slot], dx_hbm.at[tile_at(i)], sems.at[8 + slot])

    def row_read(i):
        return pltpu.make_async_copy(dx_hbm.at[tile_at(i)], row_buf.at[i % 2], sems.at[12 + i % 2])

    tiles = rows // tile

    @pl.loop(0, tiles)
    def _(i):
        at = pl.multiple_of(i * tile, tile)
        here = pl.ds(pl.multiple_of(LEFT + at, 16), tile)
        layer, dhid, da = feed(tok[pl.ds(at, tile), :], cot[pl.ds(at, tile), :], att[here, :], True)
        datt[here, :] = da

        @pl.when(i >= 2)
        def _():
            layer_write(i - 2).wait()
            row_write(i - 2, 0).wait()

        out_buf[i % 2] = layer.astype(BF16)
        row_buf[i % 2] = dhid
        layer_write(i).start()
        row_write(i, 0).start()

    sides = jnp.concatenate([att[pl.ds(0, LEFT), :], att[pl.ds(LEFT + rows, RIGHT), :]], axis=0)
    da = feed(tokh[...], coth[...], sides, False)
    datt[pl.ds(0, LEFT), :] = da[:LEFT]
    datt[pl.ds(LEFT + rows, RIGHT), :] = da[LEFT:]

    if packs:

        @pl.loop(0, second.shape[0] // 4)
        def _(i):
            pack_second(i, gwo, gwu, second)

        pack_down(gwd, second)
        second_sent = pltpu.make_async_copy(second, second_hbm, sems.at[14])
        second_sent.start()

    for i in (tiles - 2, tiles - 1):
        row_write(i, 0).wait()
    row_read(0).start()
    gw[...] = jnp.zeros(gw.shape, F32)

    @pl.loop(0, count)
    def _(i):
        attention_backward(i, starts, ends, qkv, probs, att, datt, dqkv, gsum, width, rows)

    @pl.loop(0, tiles)
    def _(i):
        at = pl.multiple_of(i * tile, tile)
        row_read(i).wait()

        @pl.when(i + 1 < tiles)
        def _():
            row_read(i + 1).start()

        @pl.when(i >= 2)
        def _():
            row_write(i - 2, 2).wait()

        d = dqkv[pl.ds(pl.multiple_of(LEFT + at, 16), tile), :]
        xhat, inverse = normed(tok[pl.ds(at, tile), :].astype(F32))
        n1 = (xhat * g1 + b1).astype(BF16)
        gw[...] += dot(n1.T, d)
        dn1 = dot_nt(d, wqkv[...])
        for j, x in ((1, d[:, 2 * width :].astype(F32)), (4, dn1 * xhat), (5, dn1)):
            gsum[j : j + 1, :] += colsum(x)
        row_buf[2 + i % 2] = row_buf[i % 2] + norm_back(dn1, xhat, inverse, g1)
        row_write(i, 2).start()

    if packs:

        @pl.loop(0, first.shape[0] // 4)
        def _(i):
            pack_first(i, gw, first)

        pack_small(gsum[...], gupb[...], first)
        first_sent = pltpu.make_async_copy(first, first_hbm, sems.at[15])
        first_sent.start()
        first_sent.wait()
        second_sent.wait()
    for i in (tiles - 2, tiles - 1):
        layer_write(i).wait()
        row_write(i, 2).wait()


def middle(packs, start, end, qkv, qkvh, tok, tokh, cot, coth, wqkv, wo, wu, wd, vec, upb):
    rows, width = tok.shape
    ff = wu.shape[1]
    padded = rows + HALO + SPARE
    tile = 512
    vmem = pl.BlockSpec(memory_space=pltpu.VMEM)
    smem = pl.BlockSpec(memory_space=pltpu.SMEM)
    anyw = pl.BlockSpec(memory_space=pl.ANY)
    most = rows // SHORTEST + 4
    n = lax.axis_size(AXES)
    S = jax.ShapeDtypeStruct
    sums = [((8, width), F32), ((8, ff), F32), ((width, 3 * width), F32), ((width, width), F32), ((width, ff), F32), ((width, ff), F32)]
    slabs = [((n, 16, FIRST), BF16), ((n, 16, SECOND), BF16)]
    held = slabs + [a for i, a in enumerate(sums) if i != 2] if packs else []
    return pl.pallas_call(
        functools.partial(middle_kernel, packs),
        out_shape=[S((rows, width), BF16), S((rows, width), F32)] + [S(*a) for a in (slabs if packs else sums)],
        in_specs=[smem, smem, anyw, anyw, anyw, vmem, anyw] + [vmem] * 7,
        out_specs=[anyw, anyw] + ([anyw] * 2 if packs else [vmem] * 6),
        scratch_shapes=[pltpu.VMEM(*a) for a in held]
        + [
            pltpu.VMEM((padded, 3 * width), BF16),
            pltpu.VMEM((padded, 3 * width), BF16),
            pltpu.VMEM((padded, width // HDIM * WIN), BF16),
            pltpu.VMEM((padded, width), BF16),
            pltpu.VMEM((padded, width), BF16),
            pltpu.VMEM((rows, width), BF16),
            pltpu.VMEM((rows, width), BF16),
            pltpu.VMEM((2, tile, width), BF16),
            pltpu.VMEM((4, tile, width), F32),
            pltpu.SMEM((most,), jnp.int32),
            pltpu.SMEM((most,), jnp.int32),
            pltpu.SemaphoreType.DMA((16,)),
        ],
        compiler_params=pltpu.CompilerParams(vmem_limit_bytes=VMEM_BYTES),
        name="middle",
    )(start, end, qkv, qkvh, tok, tokh, cot, coth, wqkv, wo, wu, wd, vec, upb)


COLS, ROWS_UP, LAYERS, CORES = 2, 2, 4, 2
LANES = 3584
SMALL, QKV, OUT, UP, DOWN = 0, 128, 1280, 1664, 2432
SPLIT = 768
PIECES = ((0, 1280, 1), (1280, 2176, 1), (2176, 3072, 1), (3072, 3584, 0))
MESH = pl.DeviceIdType.MESH


def here():
    dp, fs = lax.axis_index("dp"), lax.axis_index("fsdp")
    return dp // CORES, dp % CORES, fs // ROWS_UP, fs % ROWS_UP


def place(x, c, z, y):
    return (x * CORES + c, z * ROWS_UP + y)


def number(x, c, z, y):
    return (x * CORES + c) * (LAYERS * ROWS_UP) + z * ROWS_UP + y


def greet(ids):
    barrier = pltpu.get_barrier_semaphore()
    for d in ids:
        pl.semaphore_signal(barrier, inc=1, device_id=d, device_id_type=MESH)
    pl.semaphore_wait(barrier, len(ids))


def remote(src, dst, send, recv, to):
    return pltpu.make_async_remote_copy(src_ref=src, dst_ref=dst, send_sem=send, recv_sem=recv, device_id=to, device_id_type=MESH)


def along(step):
    dp, fs = lax.axis_size("dp"), lax.axis_size("fsdp")
    at = lax.rem(lax.axis_index("dp") * fs + lax.axis_index("fsdp") + step + dp * fs, dp * fs)
    return (at // fs, lax.rem(at, fs))


class Gather:
    def __init__(self, slabs, send, recv):
        self.slabs, self.send, self.recv = slabs, send, recv
        self.x, self.c, self.z, self.y = here()

    def copy(self, piece, slab, to):
        lo, hi, _ = PIECES[piece]
        ref = self.slabs.at[slab, :, lo:hi]
        return remote(ref, ref, self.send.at[piece], self.recv.at[piece, slab], to)

    def give(self, piece, slab, axes):
        x, c, z, y = self.x, self.c, self.z, self.y
        for axis in axes:
            if axis == "z":
                for d in range(1, LAYERS):
                    self.copy(piece, slab, place(x, c, lax.rem(z + d, LAYERS), y)).start()
            else:
                to = {"x": place(1 - x, c, z, y), "y": place(x, c, z, 1 - y), "c": place(x, 1 - c, z, y)}[axis]
                self.copy(piece, slab, to).start()

    def own(self, piece):
        self.give(piece, number(self.x, self.c, self.z, self.y), "zxyc")

    def take(self, piece, slab):
        self.copy(piece, slab, place(self.x, self.c, self.z, self.y)).wait_recv()

    def stage(self, piece, level):
        x, c, z, y = self.x, self.c, self.z, self.y
        order = PIECES[piece][2]
        second, third = ("x", "y") if order == 0 else ("y", "x")
        if level == 0:
            group = [(x, lax.rem(z + d, LAYERS), y) for d in range(1, LAYERS)]
            passed = second + third + "c"
        elif level == 1:
            group = [(1 - x, lax.rem(z + d, LAYERS), y) if order == 0 else (x, lax.rem(z + d, LAYERS), 1 - y) for d in range(LAYERS)]
            passed = third + "c"
        else:
            if order == 0:
                group = [(x if s == 0 else 1 - x, lax.rem(z + d, LAYERS), 1 - y) for s in range(2) for d in range(LAYERS)]
            else:
                group = [(1 - x, lax.rem(z + d, LAYERS), y if s == 0 else 1 - y) for s in range(2) for d in range(LAYERS)]
            passed = "c"
        for gx, gz, gy in group:
            slab = number(gx, c, gz, gy)
            self.take(piece, slab)
            self.give(piece, slab, passed)

    def siblings(self, piece):
        x, c, z, y = self.x, self.c, self.z, self.y
        for dx in range(COLS):
            for dy in range(ROWS_UP):
                for d in range(LAYERS):
                    self.take(piece, number(x if dx == 0 else 1 - x, 1 - c, lax.rem(z + d, LAYERS), y if dy == 0 else 1 - y))

    def finish(self, piece):
        lo, hi, _ = PIECES[piece]
        ref = self.slabs.at[pl.ds(0, 31), :, lo:hi]
        remote(ref, ref, self.send.at[piece], self.recv.at[piece, 0], place(self.x, self.c, self.z, self.y)).wait_send()


def unpack_first(i, slabs, wqkv):
    parts = [slabs[4 * i + d, :12, QKV:OUT].astype(F32) for d in range(4)]
    wqkv[pl.ds(pl.multiple_of(48 * i, 16), 48), :] = jnp.concatenate(parts, axis=0).astype(BF16)


def unpack_rest(i, slabs, wo, wu, wd):
    width, split = wo.shape[1], SPLIT
    at = pl.ds(pl.multiple_of(48 * i, 16), 48)
    parts = [slabs[4 * i + d, :, OUT:DOWN].astype(F32) for d in range(4)]
    full = jnp.concatenate([p[:12] for p in parts], axis=0).astype(BF16)
    wo[at, :] = full[:, : UP - OUT]
    wu[at, :split] = full[:, UP - OUT :]
    spare = [slabs[4 * i + d, :, QKV:DOWN].astype(F32)[12:] for d in range(4)]
    wu[at, split:] = jnp.concatenate([p[:, split * j : split * (j + 1)] for p in spare for j in range(3)], axis=0).astype(BF16)
    for d in range(4):
        for j in range(3):
            wd[pl.ds(pl.multiple_of(48 * (4 * i + d) + 16 * j, 16), 16), :] = slabs[4 * i + d, :, DOWN + width * j : DOWN + width * (j + 1)]


def unpack_small(slabs, vec, upb):
    lane = lax.broadcasted_iota(jnp.int32, (8, 128), 1)
    lines = [jnp.zeros((8, 128), F32) for _ in range(vec.shape[1] // 128)]
    ups = [jnp.zeros((8, 128), F32) for _ in range(upb.shape[1] // 128)]
    for k in range(slabs.shape[0]):
        s = slabs[k, :, SMALL:QKV].astype(F32)
        for tiles, block, size in ((lines, s[:8], 12), (ups, s[8:], 48)):
            t, by = divmod(size * k, 128)
            moved = pltpu.roll(block, by, 1) if by else block
            if by + size <= 128:
                tiles[t] = tiles[t] + moved
            else:
                tiles[t] = tiles[t] + jnp.where(lane >= by, moved, 0.0)
                tiles[t + 1] = tiles[t + 1] + jnp.where(lane < by, moved, 0.0)
    vec[...] = jnp.concatenate(lines, axis=1)
    upb[...] = jnp.concatenate(ups, axis=1)


def gather_kernel(
    small, wqkv_in, wo_in, wu_in, wd_in, tok, cot,
    wqkv, wo, wu, wd, vec, upb, tokh, coth, qkv, qkvh,
    slabs, tok_v, tokh_v, tile_v, send, recv, side_send, side_recv, sems,
):
    x, c, z, y = here()
    me = number(x, c, z, y)
    rows, width = tok.shape
    n = slabs.shape[0]
    load = pltpu.make_async_copy(tok, tok_v, sems.at[0])
    load.start()
    own = slabs.at[me]
    own[:, SMALL:QKV] = small[...]
    up = wu_in[...].astype(F32)
    top = jnp.concatenate([wqkv_in[...].astype(F32), wo_in[...].astype(F32), up[:, :SPLIT]], axis=1)
    rest = jnp.concatenate([up[4 * i : 4 * i + 4, SPLIT:] for i in range(3)], axis=1)
    own[:, QKV:DOWN] = jnp.concatenate([top, rest], axis=0).astype(BF16)
    for i in range(3):
        own[:, DOWN + width * i : DOWN + width * (i + 1)] = wd_in[16 * i : 16 * i + 16, :]

    greet(
        [place(x, c, lax.rem(z + d, LAYERS), y) for d in range(1, LAYERS)]
        + [place(1 - x, c, z, y), place(x, c, z, 1 - y), place(x, 1 - c, z, y), along(1), along(-1)]
    )
    g = Gather(slabs, send, recv)
    g.own(0)
    sides = []
    for j, (src, dst) in enumerate(((tok, tokh_v), (cot, coth))):
        sides.append(remote(src.at[pl.ds(rows - LEFT, LEFT)], dst.at[pl.ds(0, LEFT)], side_send.at[2 * j], side_recv.at[2 * j], along(1)))
        sides.append(remote(src.at[pl.ds(0, RIGHT)], dst.at[pl.ds(LEFT, RIGHT)], side_send.at[2 * j + 1], side_recv.at[2 * j + 1], along(-1)))
    for p in (1, 2, 3):
        g.own(p)
    for p in range(4):
        g.stage(p, 0)
    g.stage(0, 1)
    for s in sides:
        s.start()
    for p in (1, 2, 3):
        g.stage(p, 1)
    g.stage(0, 2)
    g.siblings(0)

    @pl.loop(0, n // 4)
    def _(i):
        unpack_first(i, slabs, wqkv)

    unpack_small(slabs, vec, upb)
    load.wait()
    tile = tile_v.shape[1]

    def write(i):
        return pltpu.make_async_copy(tile_v.at[i % 2], qkv.at[pl.ds(tile * i, tile)], sems.at[1 + i % 2])

    gain, shift = vec[4:5, :], vec[5:6, :]
    bias = jnp.concatenate([vec[0:1, :], jnp.zeros((1, width), F32), vec[1:2, :]], axis=1)
    steps = [lambda p=p: g.stage(p, 2) for p in (1, 2, 3)]
    for i in range(rows // tile):
        if i < len(steps):
            steps[i]()
        if i >= 2:
            write(i - 2).wait()
        tile_v[i % 2] = qkv_rows(tok_v[pl.ds(tile * i, tile), :], wqkv[...], gain, shift, bias, width)
        write(i).start()
    for p in (1, 2, 3):
        g.siblings(p)

    @pl.loop(0, n // 4)
    def _(i):
        unpack_rest(i, slabs, wo, wu, wd)

    for s in sides:
        s.wait()
    last = rows // tile
    write(last - 2).wait()
    tile_v[last % 2, :HALO] = qkv_rows(tokh_v[...], wqkv[...], gain, shift, bias, width)
    ends = [
        pltpu.make_async_copy(tile_v.at[last % 2, pl.ds(0, HALO)], qkvh, sems.at[3]),
        pltpu.make_async_copy(tokh_v, tokh, sems.at[4]),
    ]
    for e in ends:
        e.start()
    for p in range(4):
        g.finish(p)
    write(last - 1).wait()
    for e in ends:
        e.wait()


def gather_all(small, wqkv, wo, wu, wd, tok, cot):
    n = lax.axis_size(AXES)
    rows, width = tok.shape
    vmem = pl.BlockSpec(memory_space=pltpu.VMEM)
    anyw = pl.BlockSpec(memory_space=pl.ANY)
    S = jax.ShapeDtypeStruct
    return pl.pallas_call(
        gather_kernel,
        out_shape=(
            S((width, wqkv.shape[1]), BF16), S((width, width), BF16), S((width, wu.shape[1]), BF16), S((wd.shape[0] * n, width), BF16),
            S((8, width), F32), S((8, wu.shape[1]), F32), S((HALO, width), BF16), S((HALO, width), BF16),
            S((rows, wqkv.shape[1]), BF16), S((HALO, wqkv.shape[1]), BF16),
        ),
        in_specs=[vmem] * 5 + [anyw] * 2,
        out_specs=(vmem,) * 6 + (anyw,) * 4,
        scratch_shapes=[
            pltpu.VMEM((n, 16, LANES), BF16),
            pltpu.VMEM((rows, width), BF16),
            pltpu.VMEM((HALO, width), BF16),
            pltpu.VMEM((2, 512, wqkv.shape[1]), BF16),
            pltpu.SemaphoreType.DMA((4,)),
            pltpu.SemaphoreType.DMA((4, n)),
            pltpu.SemaphoreType.DMA((4,)),
            pltpu.SemaphoreType.DMA((4,)),
            pltpu.SemaphoreType.DMA((5,)),
        ],
        compiler_params=pltpu.CompilerParams(collective_id=0, has_side_effects=True, vmem_limit_bytes=VMEM_BYTES),
        name="gather",
    )(small, wqkv, wo, wu, wd, tok, cot)


FIRST, SECOND = 1024, 2688
SPARE_QKV, SPARE_UP = 896, 1152
DOWN_AT = 1536
SHARES = (
    (1, 0, 512, 0), (1, 512, 1024, 1), (1, 1024, 1408, 0), (1, 1408, 1792, 1), (1, 1792, 2304, 0), (1, 2304, 2688, 1), (0, 0, 512, 0), (0, 512, 1024, 1),
)


def pack_first(i, gw, out):
    x = gw[pl.ds(pl.multiple_of(48 * i, 16), 48), :]
    for d in range(4):
        part = x[12 * d : 12 * d + 12]
        rest = jnp.concatenate([part[4 * j : 4 * j + 4, SPARE_QKV:] for j in range(3)] + [jnp.zeros((4, 128), F32)], axis=1)
        out[4 * i + d, :, 128:] = jnp.concatenate([part[:, :SPARE_QKV], rest], axis=0).astype(BF16)


def pack_second(i, gwo, gwu, out):
    at = pl.ds(pl.multiple_of(48 * i, 16), 48)
    x = jnp.concatenate([gwo[at, :], gwu[at, :]], axis=1)
    width = gwo.shape[1]
    for d in range(4):
        part = x[12 * d : 12 * d + 12]
        rest = jnp.concatenate([part[4 * j : 4 * j + 4, DOWN_AT:] for j in range(3)] + [jnp.zeros((4, width), F32)], axis=1)
        out[4 * i + d, :, :DOWN_AT] = jnp.concatenate([part[:, :DOWN_AT], rest], axis=0).astype(BF16)


def pack_down(gwd, out):
    width, ff = gwd.shape
    for b in range(ff // 128):
        turned = gwd[:, 128 * b : 128 * b + 128].T.astype(BF16)
        for r in range(8):
            k, i = divmod(8 * b + r, 3)
            out[k, :, DOWN_AT + width * i : DOWN_AT + width * (i + 1)] = turned[16 * r : 16 * r + 16]


def pack_small(vectors, wide, out):
    lane = lax.broadcasted_iota(jnp.int32, (8, 128), 1)
    for k in range(out.shape[0]):
        blocks = []
        for src, size in ((vectors, 12), (wide, 48)):
            t, by = divmod(size * k, 128)
            block = src[:, 128 * t : 128 * t + 128]
            if by:
                block = pltpu.roll(block, 128 - by, 1)
                if by + size > 128:
                    block = jnp.where(lane < 128 - by, block, pltpu.roll(src[:, 128 * t + 128 : 128 * t + 256], 128 - by, 1))
            blocks.append(block)
        out[k, :, 0:128] = jnp.concatenate(blocks, axis=0).astype(BF16)


class Scatter:
    def __init__(self, share, parts, mine, others, first, second, third, sems):
        self.block, self.lo, self.hi, self.order = SHARES[share]
        self.share, self.parts = share, parts[self.block]
        self.sum, self.core, self.first, self.second, self.third = mine, others, first, second, third
        self.send, self.core_sem, self.first_sem, self.second_sem, self.third_sem = sems
        self.x, self.c, self.z, self.y = here()
        self.lanes = slice(self.lo, self.hi)
        self.wide = slice(0, self.hi - self.lo)

    def part(self, da, db, d, core):
        dx, dy = (db, da) if self.order == 0 else (da, db)
        slab = number(1 - self.x if dx else self.x, core, lax.rem(self.z + d, LAYERS), 1 - self.y if dy else self.y)
        return self.parts.at[slab, :, self.lanes]

    def move(self, src, dst, sem, to):
        return remote(src, dst, self.send.at[self.share], sem, to)

    def slot(self, da, db, d):
        return (da * 2 + db) * LAYERS + d

    def to_core(self, da, db, d):
        s = self.slot(da, db, d)
        to = place(self.x, 1 - self.c, self.z, self.y)
        return self.move(self.part(da, db, d, 1 - self.c), self.core.at[self.share, s, :, self.wide], self.core_sem.at[self.share, s], to)

    def to_first(self, db, d):
        s = self.slot(1, db, d)
        to = place(self.x, self.c, self.z, 1 - self.y) if self.order == 0 else place(1 - self.x, self.c, self.z, self.y)
        at = db * LAYERS + d
        return self.move(self.sum.at[self.share, s, :, self.wide], self.first.at[self.share, at, :, self.wide], self.first_sem.at[self.share, at], to)

    def to_second(self, d):
        s = self.slot(0, 1, d)
        to = place(1 - self.x, self.c, self.z, self.y) if self.order == 0 else place(self.x, self.c, self.z, 1 - self.y)
        return self.move(self.sum.at[self.share, s, :, self.wide], self.second.at[self.share, d, :, self.wide], self.second_sem.at[self.share, d], to)

    def to_third(self, d):
        s = self.slot(0, 0, d)
        to = place(self.x, self.c, lax.rem(self.z + d, LAYERS), self.y)
        return self.move(self.sum.at[self.share, s, :, self.wide], self.third.at[self.share, d - 1, :, self.wide], self.third_sem.at[self.share, d - 1], to)

    def begin(self):
        for da, db in ((1, 1), (1, 0), (0, 1), (0, 0)):
            for d in (1, 2, 3, 0):
                self.to_core(da, db, d).start()

    def total(self, da, db, d):
        s = self.slot(da, db, d)
        self.to_core(da, db, d).wait_recv()
        t = self.part(da, db, d, self.c)[...].astype(F32) + self.core[self.share, s, :, self.wide].astype(F32)
        if da == 0:
            self.to_first(db, d).wait_recv()
            t = t + self.first[self.share, db * LAYERS + d, :, self.wide].astype(F32)
            if db == 0:
                self.to_second(d).wait_recv()
                t = t + self.second[self.share, d, :, self.wide].astype(F32)
        return t

    def level(self, n):
        for da, db, d in {
            0: [(1, db, d) for db in (1, 0) for d in (1, 2, 3, 0)],
            1: [(0, 1, d) for d in (1, 2, 3, 0)],
            2: [(0, 0, d) for d in (1, 2, 3)],
        }[n]:
            self.sum[self.share, self.slot(da, db, d), :, self.wide] = self.total(da, db, d).astype(BF16)
            (self.to_first(db, d) if n == 0 else self.to_second(d) if n == 1 else self.to_third(d)).start()

    def result(self):
        t = self.total(0, 0, 0)
        for d in (1, 2, 3):
            self.to_third(d).wait_recv()
            t = t + self.third[self.share, d - 1, :, self.wide].astype(F32)
        return t

    def finish(self):
        ref = self.parts.at[pl.ds(0, 31), :, self.lanes]
        self.move(ref, ref, self.core_sem.at[self.share, 0], place(self.x, self.c, self.z, self.y)).wait_send()


def scatter_kernel(first_in, second_in, one, two, mine, core, first, second, third, *sems):
    x, c, z, y = here()
    greet(
        [place(x, c, lax.rem(z + d, LAYERS), y) for d in range(1, LAYERS)]
        + [place(1 - x, c, z, y), place(x, c, z, 1 - y), place(x, 1 - c, z, y)]
    )
    shares = [Scatter(i, (first_in, second_in), mine, core, first, second, third, sems) for i in range(len(SHARES))]
    for s in shares:
        s.begin()
    pairs = len(shares) // 2
    for step in range(pairs + 2):
        for n in range(3):
            if 0 <= step - n < pairs:
                for s in shares[2 * (step - n) : 2 * (step - n) + 2]:
                    s.level(n)
    for s in shares:
        (two if s.block else one)[:, s.lanes] = s.result()
    for s in shares:
        s.finish()


def finish_kernel(one, two, gqkv, gwo, gwu, gwd, ups, *smalls):
    width, own = gwo.shape[1], gwo.shape[0]
    gqkv[:, :SPARE_QKV] = one[:own, 128:]
    gwo[...] = two[:own, :width]
    gwu[:, :SPARE_UP] = two[:own, width:DOWN_AT]
    for j in range(3):
        gqkv[4 * j : 4 * j + 4, SPARE_QKV:] = one[own:, 128 + 256 * j : 128 + 256 * (j + 1)]
        gwu[4 * j : 4 * j + 4, SPARE_UP:] = two[own:, width * j : width * (j + 1)]
        gwd[16 * j : 16 * j + 16, :] = two[:, DOWN_AT + width * j : DOWN_AT + width * (j + 1)]
    ups[...] = one[8, : ups.shape[0]]
    for j, ref in enumerate(smalls):
        ref[...] = one[j, :own]


def finish(one, two, width, ff):
    n = lax.axis_size(AXES)
    own = width // n
    S = jax.ShapeDtypeStruct
    shapes = [(own, 3 * width), (own, width), (own, ff), (ff // n, width), (ff // n,)] + [(own,)] * 8
    return pl.pallas_call(finish_kernel, out_shape=[S(a, F32) for a in shapes], name="finish")(one, two)


def scatter_all(first, second):
    vmem = pl.BlockSpec(memory_space=pltpu.VMEM)
    S = jax.ShapeDtypeStruct
    k = len(SHARES)
    widest = max(hi - lo for _, lo, hi, _ in SHARES)
    return pl.pallas_call(
        scatter_kernel,
        out_shape=(S((16, FIRST), F32), S((16, SECOND), F32)),
        in_specs=[vmem, vmem],
        out_specs=(vmem,) * 2,
        scratch_shapes=[
            pltpu.VMEM((k, 16, 16, widest), BF16),
            pltpu.VMEM((k, 16, 16, widest), BF16),
            pltpu.VMEM((k, 8, 16, widest), BF16),
            pltpu.VMEM((k, 4, 16, widest), BF16),
            pltpu.VMEM((k, 3, 16, widest), BF16),
            pltpu.SemaphoreType.DMA((k,)),
            pltpu.SemaphoreType.DMA((k, 16)),
            pltpu.SemaphoreType.DMA((k, 8)),
            pltpu.SemaphoreType.DMA((k, 4)),
            pltpu.SemaphoreType.DMA((k, 3)),
        ],
        compiler_params=pltpu.CompilerParams(collective_id=1, has_side_effects=True, vmem_limit_bytes=VMEM_BYTES),
        name="scatter",
    )(first, second)


def small_parameters(vectors, wide):
    block = jnp.stack(list(vectors), axis=0)
    block = jnp.pad(block, ((0, 0), (0, 128 - block.shape[1])))
    return jnp.concatenate([block, jnp.pad(wide[None, :], ((0, 7), (0, 128 - wide.shape[0])))], axis=0)


def per_device(
    tokens, cotangent, image_start, image_end, qkv_weight, q_bias, v_bias, out_weight, out_bias, up_weight, up_bias,
    down_weight, down_bias, first_gain, first_bias, second_gain, second_bias,
):
    width, ff = tokens.shape[1], up_weight.shape[1]
    vectors = (q_bias, v_bias, out_bias, down_bias, first_gain, first_bias, second_gain, second_bias)
    packs = lax.axis_size("dp") == COLS * CORES and lax.axis_size("fsdp") == LAYERS * ROWS_UP
    if packs:
        small = small_parameters(vectors, up_bias)
        wqkv, wo, wu, wd, vec, upb, tokh, coth, qkv, qkvh = gather_all(
            small, qkv_weight, out_weight, up_weight, down_weight, tokens, cotangent
        )
    else:
        whole = lambda a: lax.all_gather(a, AXES, axis=0, tiled=True)
        wqkv, wo, wu, wd = (whole(a) for a in (qkv_weight, out_weight, up_weight, down_weight))
        vec = jnp.stack([whole(a).astype(F32) for a in vectors])
        upb = jnp.broadcast_to(whole(up_bias).astype(F32)[None, :], (8, ff))
        n = lax.axis_size(AXES)
        up, down = [(i, i + 1) for i in range(n - 1)], [(i + 1, i) for i in range(n - 1)]
        side = lambda a: jnp.concatenate([lax.ppermute(a[a.shape[0] - LEFT :], AXES, up), lax.ppermute(a[:RIGHT], AXES, down)])
        tokh, coth = side(tokens), side(cotangent)
        qkv, qkvh = project(tokens, tokh, wqkv, vec)
    layer, dx, *grads = middle(
        packs, image_start, image_end, qkv, qkvh, tokens, tokh, cotangent, coth, wqkv, wo, wu, wd, vec, upb
    )
    if packs:
        gqkv, gwo, gwu, gwd, ups, *sums = finish(*scatter_all(*grads), width, ff)
    else:
        reduced = lambda a: lax.psum_scatter(a, AXES, scatter_dimension=0, tiled=True)
        sums, ups = reduced(grads[0].T).T, reduced(grads[1][0])
        gqkv, gwo, gwu, gwd = (reduced(a) for a in (grads[2], grads[3], grads[4], grads[5].T))
    return (
        layer, dx, gqkv, sums[0], sums[1], gwo, sums[2], gwu, ups, gwd, sums[3], sums[4], sums[5], sums[6], sums[7],
    )


def solution(mesh):
    both = P(AXES, None)
    one = P(AXES)
    in_specs = (both, both, one, one, both, one, one, both, one, both, one, both, one, one, one, one, one)
    out_specs = (both, both, both, one, one, both, one, both, one, both, one, one, one, one, one)
    return jax.shard_map(per_device, mesh=mesh, in_specs=in_specs, out_specs=out_specs, check_vma=False)
```

```python
import functools
import math

import jax
import jax.numpy as jnp
from jax import lax
from jax.experimental import pallas as pl
from jax.experimental.pallas import tpu as pltpu
from jax.sharding import PartitionSpec as P

F32 = jnp.float32
BF16 = jnp.bfloat16
HDIM = 64
EPS = 1e-06
NEG = -1e30
ROOT_HALF = 0.7071067811865476
GAUSS = 0.3989422804014327
LEFT = 112
RIGHT = 160
HALO = LEFT + RIGHT
KEYS = 224
WIN = 256
AHEAD = 4
SPARE = 64
SHORTEST, LONGEST = 98, 197
AXES = ("dp", "fsdp")
VMEM_BYTES = 63 * 1024 * 1024


def dot(a, b):
    return jnp.dot(a, b, preferred_element_type=F32)


def dot_nt(a, b):
    return lax.dot_general(a, b, (((1,), (1,)), ((), ())), preferred_element_type=F32)


def dot_tn(a, b):
    return lax.dot_general(a, b, (((0,), (0,)), ((), ())), preferred_element_type=F32)


def normed(x):
    centre = x - jnp.mean(x, axis=-1, keepdims=True)
    inverse = lax.rsqrt(jnp.mean(centre * centre, axis=-1, keepdims=True) + EPS)
    return centre * inverse, inverse


def norm_back(grad, xhat, inverse, gain):
    e = grad * gain
    return inverse * (
        e - jnp.mean(e, axis=-1, keepdims=True) - xhat * jnp.mean(e * xhat, axis=-1, keepdims=True)
    )


def colsum(x):
    return jnp.sum(x, axis=0, keepdims=True)


def qkv_rows(rows, weight, gain, shift, bias, width):
    xhat, _ = normed(rows.astype(F32))
    n1 = (xhat * gain + shift).astype(BF16)
    out = dot(n1, weight) + bias
    return jnp.concatenate([out[:, :width] * (1.0 / math.sqrt(HDIM)), out[:, width:]], axis=1).astype(BF16)


def qkv_kernel(tok, tokh, weight, vec, out, outh):
    width = tok.shape[1]
    gain, shift = vec[4:5, :], vec[5:6, :]
    bias = jnp.concatenate([vec[0:1, :], jnp.zeros((1, width), F32), vec[1:2, :]], axis=1)
    out[...] = qkv_rows(tok[...], weight[...], gain, shift, bias, width)

    @pl.when(pl.program_id(0) == pl.num_programs(0) - 1)
    def _():
        outh[...] = qkv_rows(tokh[...], weight[...], gain, shift, bias, width)


def project(tok, tokh, weight, vec):
    rows, width = tok.shape
    tile = 512
    whole = lambda a: pl.BlockSpec(a.shape, lambda i: (0, 0))
    wide = weight.shape[1]
    return pl.pallas_call(
        qkv_kernel,
        grid=(rows // tile,),
        out_shape=(jax.ShapeDtypeStruct((rows, wide), BF16), jax.ShapeDtypeStruct((HALO, wide), BF16)),
        in_specs=[pl.BlockSpec((tile, width), lambda i: (i, 0))] + [whole(a) for a in (tokh, weight, vec)],
        out_specs=(pl.BlockSpec((tile, wide), lambda i: (i, 0)), pl.BlockSpec((HALO, wide), lambda i: (0, 0))),
        name="project",
    )(tok, tokh, weight, vec)


def image_bounds(i, starts, ends):
    s, e = starts[i], ends[i]
    a = pl.multiple_of((s // 16) * 16, 16)
    return s, e, a


def put(ref, a, columns, value, first_row):
    rows = value.shape[0]
    old = ref[pl.ds(a, 16), columns].astype(F32)
    row = lax.broadcasted_iota(jnp.int32, (16, value.shape[1]), 0) + a
    ref[pl.ds(a, 16), columns] = jnp.where(row >= first_row, value[:16].astype(F32), old).astype(ref.dtype)
    ref[pl.ds(a + 16, rows - 16), columns] = value[16:].astype(ref.dtype)


def lane_masks(rows):
    lane = lax.broadcasted_iota(jnp.int32, (rows, 128), 1)
    low = jnp.where(lane < HDIM, 1.0, 0.0)
    return low.astype(BF16), (1.0 - low).astype(BF16)


def attention_forward(images, starts, ends, qkv, probs, att, width):
    masks = lane_masks(KEYS)
    sides = []
    for i in images:
        s, e, a = image_bounds(i, starts, ends)
        row = lax.broadcasted_iota(jnp.int32, (KEYS, 1), 0) + a
        key_bias = jnp.where((row >= s) & (row < e), 0.0, NEG)
        col = lax.broadcasted_iota(jnp.int32, (1, WIN), 1) + a
        query_on = jnp.where((col >= s) & (col < e), 1.0, 0.0)
        sides.append((s, a, key_bias, query_on))

    def scores_of(image, head):
        s, a, key_bias, _ = sides[image]
        pair, half = divmod(head, 2)
        q = qkv[pl.ds(a, WIN), 128 * pair : 128 * pair + 128]
        k = qkv[pl.ds(a, KEYS), width + 128 * pair : width + 128 * pair + 128]
        return dot_nt(k * masks[half], q)

    steps = [(image, 2 * pair + half) for pair in range(width // 128) for half in range(2) for image in range(len(images))]
    ready = [scores_of(*step) for step in steps[:AHEAD]]
    total = [None] * len(images)
    for n, (image, head) in enumerate(steps):
        s, a, key_bias, query_on = sides[image]
        pair, half = divmod(head, 2)
        if n + AHEAD < len(steps):
            ready.append(scores_of(*steps[n + AHEAD]))
        scores = ready[n]
        scores = jnp.concatenate([scores[:16] + key_bias[:16], scores[16:96], scores[96:] + key_bias[96:]], axis=0)
        top = jnp.max(scores, axis=0, keepdims=True)
        ex = jnp.exp(scores - top)
        p = (ex * (query_on / jnp.sum(ex, axis=0, keepdims=True))).astype(BF16)
        put(probs, a, slice(WIN * head, WIN * head + WIN), p, s)
        v = qkv[pl.ds(a, KEYS), 2 * width + 128 * pair : 2 * width + 128 * pair + 128]
        part = dot_tn(p, v * masks[half])
        total[image] = part if half == 0 else total[image] + part
        if half == 1:
            put(att, a, slice(128 * pair, 128 * pair + 128), total[image], s)


def attention_backward(images, fresh, starts, ends, qkv, probs, att, datt, dqkv, gvec, width, rows):
    scale = 1.0 / math.sqrt(HDIM)
    masks, wide_masks = lane_masks(KEYS), lane_masks(WIN)
    group = lax.broadcasted_iota(jnp.int32, (8, width), 1) // HDIM
    heads = jnp.where(group == lax.broadcasted_iota(jnp.int32, (8, width), 0), 1.0, 0.0).astype(BF16)
    sides = []
    for i, on in zip(images, fresh):
        s, e, a = image_bounds(i, starts, ends)
        row = lax.broadcasted_iota(jnp.int32, (KEYS, 128), 0) + a
        inside = jnp.where((row >= s) & (row < e), 1.0, 0.0).astype(BF16)
        query = lax.broadcasted_iota(jnp.int32, (WIN, 128), 0) + a
        own = jnp.where((query >= LEFT) & (query < LEFT + rows), on, 0.0)
        both = att[pl.ds(a, WIN), :].astype(F32) * datt[pl.ds(a, WIN), :].astype(F32)
        high = both.astype(BF16)
        delta = dot_nt(heads, high) + dot_nt(heads, (both - high.astype(F32)).astype(BF16))
        sides.append((s, a, inside, own, delta))

    def dprobs_of(image, head):
        s, a, _, _, _ = sides[image]
        pair, half = divmod(head, 2)
        v = qkv[pl.ds(a, KEYS), 2 * width + 128 * pair : 2 * width + 128 * pair + 128]
        return dot_nt(v * masks[half], datt[pl.ds(a, WIN), 128 * pair : 128 * pair + 128])

    steps = [(image, 2 * pair + half) for pair in range(width // 128) for half in range(2) for image in range(len(images))]
    ready = [dprobs_of(*step) for step in steps[:AHEAD]]
    sums = [None] * len(images)
    for n, (image, head) in enumerate(steps):
        s, a, inside, own, delta = sides[image]
        pair, half = divmod(head, 2)
        if n + AHEAD < len(steps):
            ready.append(dprobs_of(*steps[n + AHEAD]))
        lanes = slice(128 * pair, 128 * pair + 128)
        klanes = slice(width + 128 * pair, width + 128 * pair + 128)
        vlanes = slice(2 * width + 128 * pair, 2 * width + 128 * pair + 128)
        p = probs[pl.ds(a, KEYS), WIN * head : WIN * head + WIN]
        ds = (p.astype(F32) * (ready[n] - delta[head : head + 1])).astype(BF16)
        parts = (
            dot_tn(ds, qkv[pl.ds(a, KEYS), klanes] * (inside * masks[half])),
            dot(ds, qkv[pl.ds(a, WIN), lanes] * wide_masks[half]),
            dot(p, datt[pl.ds(a, WIN), lanes] * wide_masks[half]),
        )
        sums[image] = parts if half == 0 else tuple(x + y for x, y in zip(sums[image], parts))
        if half == 1:
            dq, dk, dv = sums[image]
            gvec[0:1, lanes] += colsum(dq * own) * scale
            put(dqkv, a, lanes, dq * scale, s)
            put(dqkv, a, klanes, dk, s)
            put(dqkv, a, vlanes, dv, s)


def middle_kernel(
    packs, start_in, end_in, qkv_in, qkvh_in, tok_in, tokh, cot_in, coth, wqkv, wo, wu, wd, vec, upb, out_hbm, dx_hbm, *refs
):
    first_hbm, second_hbm, first, second = (None,) * 4
    if packs:
        first_hbm, second_hbm, first, second, *refs = refs
        gsum, gupb, gwo, gwu, gwd, *refs = refs
        gw = gwu.at[:, : 3 * wo.shape[0]]
    else:
        gsum, gupb, gw, gwo, gwu, gwd, *refs = refs
    qkv, dqkv, probs, att, datt, tok, cot, out_buf, row_buf, starts, ends, sems = refs
    rows, width = tok_in.shape
    ff = wu.shape[1]
    chunk = ff
    extent = rows + HALO
    tile = out_buf.shape[1]
    early = rows // 3
    copies = [
        pltpu.make_async_copy(qkvh_in.at[pl.ds(0, LEFT)], qkv.at[pl.ds(0, LEFT)], sems.at[0]),
        pltpu.make_async_copy(qkv_in.at[pl.ds(0, early)], qkv.at[pl.ds(LEFT, early)], sems.at[1]),
    ]
    rest = [
        pltpu.make_async_copy(qkv_in.at[pl.ds(early, rows - early)], qkv.at[pl.ds(LEFT + early, rows - early)], sems.at[2]),
        pltpu.make_async_copy(qkvh_in.at[pl.ds(LEFT, RIGHT)], qkv.at[pl.ds(LEFT + rows, RIGHT)], sems.at[3]),
    ]
    later = [
        pltpu.make_async_copy(tok_in, tok, sems.at[4]),
        pltpu.make_async_copy(cot_in, cot, sems.at[5]),
    ]
    for c in copies + rest + later:
        c.start()

    shift = LEFT - lax.axis_index(AXES) * rows
    starts[0] = start_in[0] + shift
    ends[0] = end_in[0] + shift

    def walk(i, n):
        here = ends[i - 1]
        more = here < LEFT + rows
        at = jnp.minimum(here - LEFT, rows - 1)
        starts[i] = here
        ends[i] = end_in[at] + shift
        return jnp.where(more, i + 1, n)

    count = lax.fori_loop(1, starts.shape[0], walk, 1)

    spare = qkv.shape[0] - extent
    qkv[pl.ds(extent, spare), :] = jnp.zeros((spare, qkv.shape[1]), BF16)
    datt[pl.ds(extent, spare), :] = jnp.zeros((spare, width), BF16)
    probs[pl.ds(0, LEFT), :] = jnp.zeros((LEFT, probs.shape[1]), BF16)
    att[pl.ds(0, LEFT), :] = jnp.zeros((LEFT, width), BF16)
    att[pl.ds(LEFT + rows, RIGHT + spare), :] = jnp.zeros((RIGHT + spare, width), BF16)
    dqkv[pl.ds(0, LEFT), :] = jnp.zeros((LEFT, dqkv.shape[1]), BF16)
    for c in copies:
        c.wait()

    assert 3 * LONGEST + WIN <= early and rows > 5 * LONGEST

    @pl.loop(0, (count + 1) // 2)
    def _(i):
        @pl.when(i == 2)
        def _():
            for c in rest:
                c.wait()

        attention_forward([2 * i, jnp.minimum(2 * i + 1, count - 1)], starts, ends, qkv, probs, att, width)

    bo, bd, g1, b1, g2, b2 = (vec[j : j + 1, :] for j in (2, 3, 4, 5, 6, 7))

    def feed(x, c, at, own):
        hid = x.astype(F32) + dot(at, wo[...]) + bo
        xhat, inverse = normed(hid)
        n2 = (xhat * g2 + b2).astype(BF16)
        down = dn2 = None
        if own:
            ct, nt = c.T, n2.T
        for f in range(0, ff, chunk):
            cols = slice(f, f + chunk)
            pre = dot(n2, wu[:, cols]) + upb[0:1, cols]
            half = 0.5 * (1.0 + lax.erf(pre * ROOT_HALF))
            slope = half + pre * jnp.exp(-0.5 * pre * pre) * GAUSS
            dpre = dot_nt(c, wd[cols, :]) * slope
            dpre_b = dpre.astype(BF16)
            part = dot_nt(dpre_b, wu[:, cols])
            dn2 = part if dn2 is None else dn2 + part
            if own:
                act = (pre * half).astype(BF16)
                part = dot(act, wd[cols, :])
                down = part if down is None else down + part
                gwd[:, cols] += dot(ct, act)
                gwu[:, cols] += dot(nt, dpre_b)
                gupb[0:1, cols] += colsum(dpre)
        dhid = c.astype(F32) + norm_back(dn2, xhat, inverse, g2)
        dhid_b = dhid.astype(BF16)
        da = dot_nt(dhid_b, wo[...]).astype(BF16)
        if own:
            gwo[...] += dot_tn(at, dhid_b)
            for j, x in ((2, dhid), (3, c.astype(F32)), (6, dn2 * xhat), (7, dn2)):
                gsum[j : j + 1, :] += colsum(x)
            return hid + down + bd, dhid, da
        return da

    gwo[...] = jnp.zeros_like(gwo)
    gwu[...] = jnp.zeros_like(gwu)
    gwd[...] = jnp.zeros_like(gwd)
    gsum[...] = jnp.zeros_like(gsum)
    gupb[...] = jnp.zeros_like(gupb)
    for c in later:
        c.wait()

    def tile_at(i):
        return pl.ds(pl.multiple_of(i * tile, tile), tile)

    def layer_write(i):
        return pltpu.make_async_copy(out_buf.at[i % 2], out_hbm.at[tile_at(i)], sems.at[6 + i % 2])

    def row_write(i, first_slot):
        slot = first_slot + i % 2
        return pltpu.make_async_copy(row_buf.at[slot], dx_hbm.at[tile_at(i)], sems.at[8 + slot])

    def row_read(i):
        return pltpu.make_async_copy(dx_hbm.at[tile_at(i)], row_buf.at[i % 2], sems.at[12 + i % 2])

    tiles = rows // tile

    @pl.loop(0, tiles)
    def _(i):
        at = pl.multiple_of(i * tile, tile)
        here = pl.ds(pl.multiple_of(LEFT + at, 16), tile)
        layer, dhid, da = feed(tok[pl.ds(at, tile), :], cot[pl.ds(at, tile), :], att[here, :], True)
        datt[here, :] = da

        @pl.when(i >= 2)
        def _():
            layer_write(i - 2).wait()
            row_write(i - 2, 0).wait()

        out_buf[i % 2] = layer.astype(BF16)
        row_buf[i % 2] = dhid
        layer_write(i).start()
        row_write(i, 0).start()

    sides = jnp.concatenate([att[pl.ds(0, LEFT), :], att[pl.ds(LEFT + rows, RIGHT), :]], axis=0)
    da = feed(tokh[...], coth[...], sides, False)
    datt[pl.ds(0, LEFT), :] = da[:LEFT]
    datt[pl.ds(LEFT + rows, RIGHT), :] = da[LEFT:]

    if packs:

        @pl.loop(0, second.shape[0] // 4)
        def _(i):
            pack_second(i, gwo, gwu, second)

        pack_down(gwd, second)
        second_sent = pltpu.make_async_copy(second, second_hbm, sems.at[14])
        second_sent.start()

    for i in (tiles - 2, tiles - 1):
        row_write(i, 0).wait()
    row_read(0).start()
    gw[...] = jnp.zeros(gw.shape, F32)

    @pl.loop(0, (count + 1) // 2)
    def _(i):
        attention_backward([2 * i, jnp.minimum(2 * i + 1, count - 1)], [1.0, jnp.where(2 * i + 1 < count, 1.0, 0.0)], starts, ends, qkv, probs, att, datt, dqkv, gsum, width, rows)

    @pl.loop(0, tiles)
    def _(i):
        at = pl.multiple_of(i * tile, tile)
        row_read(i).wait()

        @pl.when(i + 1 < tiles)
        def _():
            row_read(i + 1).start()

        @pl.when(i >= 2)
        def _():
            row_write(i - 2, 2).wait()

        d = dqkv[pl.ds(pl.multiple_of(LEFT + at, 16), tile), :]
        xhat, inverse = normed(tok[pl.ds(at, tile), :].astype(F32))
        n1 = (xhat * g1 + b1).astype(BF16)
        gw[...] += dot(n1.T, d)
        dn1 = dot_nt(d, wqkv[...])
        for j, x in ((1, d[:, 2 * width :].astype(F32)), (4, dn1 * xhat), (5, dn1)):
            gsum[j : j + 1, :] += colsum(x)
        row_buf[2 + i % 2] = row_buf[i % 2] + norm_back(dn1, xhat, inverse, g1)
        row_write(i, 2).start()

    if packs:

        @pl.loop(0, first.shape[0] // 4)
        def _(i):
            pack_first(i, gw, first)

        pack_small(gsum[...], gupb[...], first)
        first_sent = pltpu.make_async_copy(first, first_hbm, sems.at[15])
        first_sent.start()
        first_sent.wait()
        second_sent.wait()
    for i in (tiles - 2, tiles - 1):
        layer_write(i).wait()
        row_write(i, 2).wait()


def middle(packs, start, end, qkv, qkvh, tok, tokh, cot, coth, wqkv, wo, wu, wd, vec, upb):
    rows, width = tok.shape
    ff = wu.shape[1]
    padded = rows + HALO + SPARE
    tile = 512
    vmem = pl.BlockSpec(memory_space=pltpu.VMEM)
    smem = pl.BlockSpec(memory_space=pltpu.SMEM)
    anyw = pl.BlockSpec(memory_space=pl.ANY)
    most = rows // SHORTEST + 4
    n = lax.axis_size(AXES)
    S = jax.ShapeDtypeStruct
    sums = [((8, width), F32), ((8, ff), F32), ((width, 3 * width), F32), ((width, width), F32), ((width, ff), F32), ((width, ff), F32)]
    slabs = [((n, 16, FIRST), BF16), ((n, 16, SECOND), BF16)]
    held = slabs + [a for i, a in enumerate(sums) if i != 2] if packs else []
    return pl.pallas_call(
        functools.partial(middle_kernel, packs),
        out_shape=[S((rows, width), BF16), S((rows, width), F32)] + [S(*a) for a in (slabs if packs else sums)],
        in_specs=[smem, smem, anyw, anyw, anyw, vmem, anyw] + [vmem] * 7,
        out_specs=[anyw, anyw] + ([anyw] * 2 if packs else [vmem] * 6),
        scratch_shapes=[pltpu.VMEM(*a) for a in held]
        + [
            pltpu.VMEM((padded, 3 * width), BF16),
            pltpu.VMEM((padded, 3 * width), BF16),
            pltpu.VMEM((padded, width // HDIM * WIN), BF16),
            pltpu.VMEM((padded, width), BF16),
            pltpu.VMEM((padded, width), BF16),
            pltpu.VMEM((rows, width), BF16),
            pltpu.VMEM((rows, width), BF16),
            pltpu.VMEM((2, tile, width), BF16),
            pltpu.VMEM((4, tile, width), F32),
            pltpu.SMEM((most,), jnp.int32),
            pltpu.SMEM((most,), jnp.int32),
            pltpu.SemaphoreType.DMA((16,)),
        ],
        compiler_params=pltpu.CompilerParams(vmem_limit_bytes=VMEM_BYTES),
        name="middle",
    )(start, end, qkv, qkvh, tok, tokh, cot, coth, wqkv, wo, wu, wd, vec, upb)


COLS, ROWS_UP, LAYERS, CORES = 2, 2, 4, 2
LANES = 3584
SMALL, QKV, OUT, UP, DOWN = 0, 128, 1280, 1664, 2432
SPLIT = 768
PIECES = ((0, 1280, 1), (1280, 2176, 1), (2176, 3072, 1), (3072, 3584, 0))
MESH = pl.DeviceIdType.MESH


def here():
    dp, fs = lax.axis_index("dp"), lax.axis_index("fsdp")
    return dp // CORES, dp % CORES, fs // ROWS_UP, fs % ROWS_UP


def place(x, c, z, y):
    return (x * CORES + c, z * ROWS_UP + y)


def number(x, c, z, y):
    return (x * CORES + c) * (LAYERS * ROWS_UP) + z * ROWS_UP + y


def greet(ids):
    barrier = pltpu.get_barrier_semaphore()
    for d in ids:
        pl.semaphore_signal(barrier, inc=1, device_id=d, device_id_type=MESH)
    pl.semaphore_wait(barrier, len(ids))


def remote(src, dst, send, recv, to):
    return pltpu.make_async_remote_copy(src_ref=src, dst_ref=dst, send_sem=send, recv_sem=recv, device_id=to, device_id_type=MESH)


def along(step):
    dp, fs = lax.axis_size("dp"), lax.axis_size("fsdp")
    at = lax.rem(lax.axis_index("dp") * fs + lax.axis_index("fsdp") + step + dp * fs, dp * fs)
    return (at // fs, lax.rem(at, fs))


class Gather:
    def __init__(self, slabs, send, recv):
        self.slabs, self.send, self.recv = slabs, send, recv
        self.x, self.c, self.z, self.y = here()

    def copy(self, piece, slab, to):
        lo, hi, _ = PIECES[piece]
        ref = self.slabs.at[slab, :, lo:hi]
        return remote(ref, ref, self.send.at[piece], self.recv.at[piece, slab], to)

    def give(self, piece, slab, axes):
        x, c, z, y = self.x, self.c, self.z, self.y
        for axis in axes:
            if axis == "z":
                for d in range(1, LAYERS):
                    self.copy(piece, slab, place(x, c, lax.rem(z + d, LAYERS), y)).start()
            else:
                to = {"x": place(1 - x, c, z, y), "y": place(x, c, z, 1 - y), "c": place(x, 1 - c, z, y)}[axis]
                self.copy(piece, slab, to).start()

    def own(self, piece):
        self.give(piece, number(self.x, self.c, self.z, self.y), "zxyc")

    def take(self, piece, slab):
        self.copy(piece, slab, place(self.x, self.c, self.z, self.y)).wait_recv()

    def stage(self, piece, level):
        x, c, z, y = self.x, self.c, self.z, self.y
        order = PIECES[piece][2]
        second, third = ("x", "y") if order == 0 else ("y", "x")
        if level == 0:
            group = [(x, lax.rem(z + d, LAYERS), y) for d in range(1, LAYERS)]
            passed = second + third + "c"
        elif level == 1:
            group = [(1 - x, lax.rem(z + d, LAYERS), y) if order == 0 else (x, lax.rem(z + d, LAYERS), 1 - y) for d in range(LAYERS)]
            passed = third + "c"
        else:
            if order == 0:
                group = [(x if s == 0 else 1 - x, lax.rem(z + d, LAYERS), 1 - y) for s in range(2) for d in range(LAYERS)]
            else:
                group = [(1 - x, lax.rem(z + d, LAYERS), y if s == 0 else 1 - y) for s in range(2) for d in range(LAYERS)]
            passed = "c"
        for gx, gz, gy in group:
            slab = number(gx, c, gz, gy)
            self.take(piece, slab)
            self.give(piece, slab, passed)

    def siblings(self, piece):
        x, c, z, y = self.x, self.c, self.z, self.y
        for dx in range(COLS):
            for dy in range(ROWS_UP):
                for d in range(LAYERS):
                    self.take(piece, number(x if dx == 0 else 1 - x, 1 - c, lax.rem(z + d, LAYERS), y if dy == 0 else 1 - y))

    def finish(self, piece):
        lo, hi, _ = PIECES[piece]
        ref = self.slabs.at[pl.ds(0, 31), :, lo:hi]
        remote(ref, ref, self.send.at[piece], self.recv.at[piece, 0], place(self.x, self.c, self.z, self.y)).wait_send()


def unpack_first(i, slabs, wqkv):
    parts = [slabs[4 * i + d, :12, QKV:OUT].astype(F32) for d in range(4)]
    wqkv[pl.ds(pl.multiple_of(48 * i, 16), 48), :] = jnp.concatenate(parts, axis=0).astype(BF16)


def unpack_rest(i, slabs, wo, wu, wd):
    width, split = wo.shape[1], SPLIT
    at = pl.ds(pl.multiple_of(48 * i, 16), 48)
    parts = [slabs[4 * i + d, :, OUT:DOWN].astype(F32) for d in range(4)]
    full = jnp.concatenate([p[:12] for p in parts], axis=0).astype(BF16)
    wo[at, :] = full[:, : UP - OUT]
    wu[at, :split] = full[:, UP - OUT :]
    spare = [slabs[4 * i + d, :, QKV:DOWN].astype(F32)[12:] for d in range(4)]
    wu[at, split:] = jnp.concatenate([p[:, split * j : split * (j + 1)] for p in spare for j in range(3)], axis=0).astype(BF16)
    for d in range(4):
        for j in range(3):
            wd[pl.ds(pl.multiple_of(48 * (4 * i + d) + 16 * j, 16), 16), :] = slabs[4 * i + d, :, DOWN + width * j : DOWN + width * (j + 1)]


def unpack_small(slabs, vec, upb):
    lane = lax.broadcasted_iota(jnp.int32, (8, 128), 1)
    lines = [jnp.zeros((8, 128), F32) for _ in range(vec.shape[1] // 128)]
    ups = [jnp.zeros((8, 128), F32) for _ in range(upb.shape[1] // 128)]
    for k in range(slabs.shape[0]):
        s = slabs[k, :, SMALL:QKV].astype(F32)
        for tiles, block, size in ((lines, s[:8], 12), (ups, s[8:], 48)):
            t, by = divmod(size * k, 128)
            moved = pltpu.roll(block, by, 1) if by else block
            if by + size <= 128:
                tiles[t] = tiles[t] + moved
            else:
                tiles[t] = tiles[t] + jnp.where(lane >= by, moved, 0.0)
                tiles[t + 1] = tiles[t + 1] + jnp.where(lane < by, moved, 0.0)
    vec[...] = jnp.concatenate(lines, axis=1)
    upb[...] = jnp.concatenate(ups, axis=1)


def gather_kernel(
    small, wqkv_in, wo_in, wu_in, wd_in, tok, cot,
    wqkv, wo, wu, wd, vec, upb, tokh, coth, qkv, qkvh,
    slabs, tok_v, tokh_v, tile_v, send, recv, side_send, side_recv, sems,
):
    x, c, z, y = here()
    me = number(x, c, z, y)
    rows, width = tok.shape
    n = slabs.shape[0]
    load = pltpu.make_async_copy(tok, tok_v, sems.at[0])
    load.start()
    own = slabs.at[me]
    own[:, SMALL:QKV] = small[...]
    up = wu_in[...].astype(F32)
    top = jnp.concatenate([wqkv_in[...].astype(F32), wo_in[...].astype(F32), up[:, :SPLIT]], axis=1)
    rest = jnp.concatenate([up[4 * i : 4 * i + 4, SPLIT:] for i in range(3)], axis=1)
    own[:, QKV:DOWN] = jnp.concatenate([top, rest], axis=0).astype(BF16)
    for i in range(3):
        own[:, DOWN + width * i : DOWN + width * (i + 1)] = wd_in[16 * i : 16 * i + 16, :]

    greet(
        [place(x, c, lax.rem(z + d, LAYERS), y) for d in range(1, LAYERS)]
        + [place(1 - x, c, z, y), place(x, c, z, 1 - y), place(x, 1 - c, z, y), along(1), along(-1)]
    )
    g = Gather(slabs, send, recv)
    g.own(0)
    sides = []
    for j, (src, dst) in enumerate(((tok, tokh_v), (cot, coth))):
        sides.append(remote(src.at[pl.ds(rows - LEFT, LEFT)], dst.at[pl.ds(0, LEFT)], side_send.at[2 * j], side_recv.at[2 * j], along(1)))
        sides.append(remote(src.at[pl.ds(0, RIGHT)], dst.at[pl.ds(LEFT, RIGHT)], side_send.at[2 * j + 1], side_recv.at[2 * j + 1], along(-1)))
    for p in (1, 2, 3):
        g.own(p)
    for p in range(4):
        g.stage(p, 0)
    g.stage(0, 1)
    for s in sides:
        s.start()
    for p in (1, 2, 3):
        g.stage(p, 1)
    g.stage(0, 2)
    g.siblings(0)

    @pl.loop(0, n // 4)
    def _(i):
        unpack_first(i, slabs, wqkv)

    unpack_small(slabs, vec, upb)
    load.wait()
    tile = tile_v.shape[1]

    def write(i):
        return pltpu.make_async_copy(tile_v.at[i % 2], qkv.at[pl.ds(tile * i, tile)], sems.at[1 + i % 2])

    gain, shift = vec[4:5, :], vec[5:6, :]
    bias = jnp.concatenate([vec[0:1, :], jnp.zeros((1, width), F32), vec[1:2, :]], axis=1)
    steps = [lambda p=p: g.stage(p, 2) for p in (1, 2, 3)]
    for i in range(rows // tile):
        if i < len(steps):
            steps[i]()
        if i >= 2:
            write(i - 2).wait()
        tile_v[i % 2] = qkv_rows(tok_v[pl.ds(tile * i, tile), :], wqkv[...], gain, shift, bias, width)
        write(i).start()
    for p in (1, 2, 3):
        g.siblings(p)

    @pl.loop(0, n // 4)
    def _(i):
        unpack_rest(i, slabs, wo, wu, wd)

    for s in sides:
        s.wait()
    last = rows // tile
    write(last - 2).wait()
    tile_v[last % 2, :HALO] = qkv_rows(tokh_v[...], wqkv[...], gain, shift, bias, width)
    ends = [
        pltpu.make_async_copy(tile_v.at[last % 2, pl.ds(0, HALO)], qkvh, sems.at[3]),
        pltpu.make_async_copy(tokh_v, tokh, sems.at[4]),
    ]
    for e in ends:
        e.start()
    for p in range(4):
        g.finish(p)
    write(last - 1).wait()
    for e in ends:
        e.wait()


def gather_all(small, wqkv, wo, wu, wd, tok, cot):
    n = lax.axis_size(AXES)
    rows, width = tok.shape
    vmem = pl.BlockSpec(memory_space=pltpu.VMEM)
    anyw = pl.BlockSpec(memory_space=pl.ANY)
    S = jax.ShapeDtypeStruct
    return pl.pallas_call(
        gather_kernel,
        out_shape=(
            S((width, wqkv.shape[1]), BF16), S((width, width), BF16), S((width, wu.shape[1]), BF16), S((wd.shape[0] * n, width), BF16),
            S((8, width), F32), S((8, wu.shape[1]), F32), S((HALO, width), BF16), S((HALO, width), BF16),
            S((rows, wqkv.shape[1]), BF16), S((HALO, wqkv.shape[1]), BF16),
        ),
        in_specs=[vmem] * 5 + [anyw] * 2,
        out_specs=(vmem,) * 6 + (anyw,) * 4,
        scratch_shapes=[
            pltpu.VMEM((n, 16, LANES), BF16),
            pltpu.VMEM((rows, width), BF16),
            pltpu.VMEM((HALO, width), BF16),
            pltpu.VMEM((2, 512, wqkv.shape[1]), BF16),
            pltpu.SemaphoreType.DMA((4,)),
            pltpu.SemaphoreType.DMA((4, n)),
            pltpu.SemaphoreType.DMA((4,)),
            pltpu.SemaphoreType.DMA((4,)),
            pltpu.SemaphoreType.DMA((5,)),
        ],
        compiler_params=pltpu.CompilerParams(collective_id=0, has_side_effects=True, vmem_limit_bytes=VMEM_BYTES),
        name="gather",
    )(small, wqkv, wo, wu, wd, tok, cot)


FIRST, SECOND = 1024, 2688
SPARE_QKV, SPARE_UP = 896, 1152
DOWN_AT = 1536
SHARES = (
    (1, 0, 512, 0), (1, 512, 1024, 1), (1, 1024, 1408, 0), (1, 1408, 1792, 1), (1, 1792, 2304, 0), (1, 2304, 2688, 1), (0, 0, 512, 0), (0, 512, 1024, 1),
)


def pack_first(i, gw, out):
    x = gw[pl.ds(pl.multiple_of(48 * i, 16), 48), :]
    for d in range(4):
        part = x[12 * d : 12 * d + 12]
        rest = jnp.concatenate([part[4 * j : 4 * j + 4, SPARE_QKV:] for j in range(3)] + [jnp.zeros((4, 128), F32)], axis=1)
        out[4 * i + d, :, 128:] = jnp.concatenate([part[:, :SPARE_QKV], rest], axis=0).astype(BF16)


def pack_second(i, gwo, gwu, out):
    at = pl.ds(pl.multiple_of(48 * i, 16), 48)
    x = jnp.concatenate([gwo[at, :], gwu[at, :]], axis=1)
    width = gwo.shape[1]
    for d in range(4):
        part = x[12 * d : 12 * d + 12]
        rest = jnp.concatenate([part[4 * j : 4 * j + 4, DOWN_AT:] for j in range(3)] + [jnp.zeros((4, width), F32)], axis=1)
        out[4 * i + d, :, :DOWN_AT] = jnp.concatenate([part[:, :DOWN_AT], rest], axis=0).astype(BF16)


def pack_down(gwd, out):
    width, ff = gwd.shape
    for b in range(ff // 128):
        turned = gwd[:, 128 * b : 128 * b + 128].T.astype(BF16)
        for r in range(8):
            k, i = divmod(8 * b + r, 3)
            out[k, :, DOWN_AT + width * i : DOWN_AT + width * (i + 1)] = turned[16 * r : 16 * r + 16]


def pack_small(vectors, wide, out):
    lane = lax.broadcasted_iota(jnp.int32, (8, 128), 1)
    for k in range(out.shape[0]):
        blocks = []
        for src, size in ((vectors, 12), (wide, 48)):
            t, by = divmod(size * k, 128)
            block = src[:, 128 * t : 128 * t + 128]
            if by:
                block = pltpu.roll(block, 128 - by, 1)
                if by + size > 128:
                    block = jnp.where(lane < 128 - by, block, pltpu.roll(src[:, 128 * t + 128 : 128 * t + 256], 128 - by, 1))
            blocks.append(block)
        out[k, :, 0:128] = jnp.concatenate(blocks, axis=0).astype(BF16)


class Scatter:
    def __init__(self, share, parts, mine, others, first, second, third, sems):
        self.block, self.lo, self.hi, self.order = SHARES[share]
        self.share, self.parts = share, parts[self.block]
        self.sum, self.core, self.first, self.second, self.third = mine, others, first, second, third
        self.send, self.core_sem, self.first_sem, self.second_sem, self.third_sem = sems
        self.x, self.c, self.z, self.y = here()
        self.lanes = slice(self.lo, self.hi)
        self.wide = slice(0, self.hi - self.lo)

    def part(self, da, db, d, core):
        dx, dy = (db, da) if self.order == 0 else (da, db)
        slab = number(1 - self.x if dx else self.x, core, lax.rem(self.z + d, LAYERS), 1 - self.y if dy else self.y)
        return self.parts.at[slab, :, self.lanes]

    def move(self, src, dst, sem, to):
        return remote(src, dst, self.send.at[self.share], sem, to)

    def slot(self, da, db, d):
        return (da * 2 + db) * LAYERS + d

    def to_core(self, da, db, d):
        s = self.slot(da, db, d)
        to = place(self.x, 1 - self.c, self.z, self.y)
        return self.move(self.part(da, db, d, 1 - self.c), self.core.at[self.share, s, :, self.wide], self.core_sem.at[self.share, s], to)

    def to_first(self, db, d):
        s = self.slot(1, db, d)
        to = place(self.x, self.c, self.z, 1 - self.y) if self.order == 0 else place(1 - self.x, self.c, self.z, self.y)
        at = db * LAYERS + d
        return self.move(self.sum.at[self.share, s, :, self.wide], self.first.at[self.share, at, :, self.wide], self.first_sem.at[self.share, at], to)

    def to_second(self, d):
        s = self.slot(0, 1, d)
        to = place(1 - self.x, self.c, self.z, self.y) if self.order == 0 else place(self.x, self.c, self.z, 1 - self.y)
        return self.move(self.sum.at[self.share, s, :, self.wide], self.second.at[self.share, d, :, self.wide], self.second_sem.at[self.share, d], to)

    def to_third(self, d):
        s = self.slot(0, 0, d)
        to = place(self.x, self.c, lax.rem(self.z + d, LAYERS), self.y)
        return self.move(self.sum.at[self.share, s, :, self.wide], self.third.at[self.share, d - 1, :, self.wide], self.third_sem.at[self.share, d - 1], to)

    def begin(self):
        for da, db in ((1, 1), (1, 0), (0, 1), (0, 0)):
            for d in (1, 2, 3, 0):
                self.to_core(da, db, d).start()

    def total(self, da, db, d):
        s = self.slot(da, db, d)
        self.to_core(da, db, d).wait_recv()
        t = self.part(da, db, d, self.c)[...].astype(F32) + self.core[self.share, s, :, self.wide].astype(F32)
        if da == 0:
            self.to_first(db, d).wait_recv()
            t = t + self.first[self.share, db * LAYERS + d, :, self.wide].astype(F32)
            if db == 0:
                self.to_second(d).wait_recv()
                t = t + self.second[self.share, d, :, self.wide].astype(F32)
        return t

    def level(self, n):
        for da, db, d in {
            0: [(1, db, d) for db in (1, 0) for d in (1, 2, 3, 0)],
            1: [(0, 1, d) for d in (1, 2, 3, 0)],
            2: [(0, 0, d) for d in (1, 2, 3)],
        }[n]:
            self.sum[self.share, self.slot(da, db, d), :, self.wide] = self.total(da, db, d).astype(BF16)
            (self.to_first(db, d) if n == 0 else self.to_second(d) if n == 1 else self.to_third(d)).start()

    def result(self):
        t = self.total(0, 0, 0)
        for d in (1, 2, 3):
            self.to_third(d).wait_recv()
            t = t + self.third[self.share, d - 1, :, self.wide].astype(F32)
        return t

    def finish(self):
        ref = self.parts.at[pl.ds(0, 31), :, self.lanes]
        self.move(ref, ref, self.core_sem.at[self.share, 0], place(self.x, self.c, self.z, self.y)).wait_send()


def scatter_kernel(first_in, second_in, one, two, mine, core, first, second, third, *sems):
    x, c, z, y = here()
    greet(
        [place(x, c, lax.rem(z + d, LAYERS), y) for d in range(1, LAYERS)]
        + [place(1 - x, c, z, y), place(x, c, z, 1 - y), place(x, 1 - c, z, y)]
    )
    shares = [Scatter(i, (first_in, second_in), mine, core, first, second, third, sems) for i in range(len(SHARES))]
    for s in shares:
        s.begin()
    pairs = len(shares) // 2
    for step in range(pairs + 2):
        for n in range(3):
            if 0 <= step - n < pairs:
                for s in shares[2 * (step - n) : 2 * (step - n) + 2]:
                    s.level(n)
    for s in shares:
        (two if s.block else one)[:, s.lanes] = s.result()
    for s in shares:
        s.finish()


def finish_kernel(one, two, gqkv, gwo, gwu, gwd, ups, *smalls):
    width, own = gwo.shape[1], gwo.shape[0]
    gqkv[:, :SPARE_QKV] = one[:own, 128:]
    gwo[...] = two[:own, :width]
    gwu[:, :SPARE_UP] = two[:own, width:DOWN_AT]
    for j in range(3):
        gqkv[4 * j : 4 * j + 4, SPARE_QKV:] = one[own:, 128 + 256 * j : 128 + 256 * (j + 1)]
        gwu[4 * j : 4 * j + 4, SPARE_UP:] = two[own:, width * j : width * (j + 1)]
        gwd[16 * j : 16 * j + 16, :] = two[:, DOWN_AT + width * j : DOWN_AT + width * (j + 1)]
    ups[...] = one[8, : ups.shape[0]]
    for j, ref in enumerate(smalls):
        ref[...] = one[j, :own]


def finish(one, two, width, ff):
    n = lax.axis_size(AXES)
    own = width // n
    S = jax.ShapeDtypeStruct
    shapes = [(own, 3 * width), (own, width), (own, ff), (ff // n, width), (ff // n,)] + [(own,)] * 8
    return pl.pallas_call(finish_kernel, out_shape=[S(a, F32) for a in shapes], name="finish")(one, two)


def scatter_all(first, second):
    vmem = pl.BlockSpec(memory_space=pltpu.VMEM)
    S = jax.ShapeDtypeStruct
    k = len(SHARES)
    widest = max(hi - lo for _, lo, hi, _ in SHARES)
    return pl.pallas_call(
        scatter_kernel,
        out_shape=(S((16, FIRST), F32), S((16, SECOND), F32)),
        in_specs=[vmem, vmem],
        out_specs=(vmem,) * 2,
        scratch_shapes=[
            pltpu.VMEM((k, 16, 16, widest), BF16),
            pltpu.VMEM((k, 16, 16, widest), BF16),
            pltpu.VMEM((k, 8, 16, widest), BF16),
            pltpu.VMEM((k, 4, 16, widest), BF16),
            pltpu.VMEM((k, 3, 16, widest), BF16),
            pltpu.SemaphoreType.DMA((k,)),
            pltpu.SemaphoreType.DMA((k, 16)),
            pltpu.SemaphoreType.DMA((k, 8)),
            pltpu.SemaphoreType.DMA((k, 4)),
            pltpu.SemaphoreType.DMA((k, 3)),
        ],
        compiler_params=pltpu.CompilerParams(collective_id=1, has_side_effects=True, vmem_limit_bytes=VMEM_BYTES),
        name="scatter",
    )(first, second)


def small_parameters(vectors, wide):
    block = jnp.stack(list(vectors), axis=0)
    block = jnp.pad(block, ((0, 0), (0, 128 - block.shape[1])))
    return jnp.concatenate([block, jnp.pad(wide[None, :], ((0, 7), (0, 128 - wide.shape[0])))], axis=0)


def per_device(
    tokens, cotangent, image_start, image_end, qkv_weight, q_bias, v_bias, out_weight, out_bias, up_weight, up_bias,
    down_weight, down_bias, first_gain, first_bias, second_gain, second_bias,
):
    width, ff = tokens.shape[1], up_weight.shape[1]
    vectors = (q_bias, v_bias, out_bias, down_bias, first_gain, first_bias, second_gain, second_bias)
    packs = lax.axis_size("dp") == COLS * CORES and lax.axis_size("fsdp") == LAYERS * ROWS_UP
    if packs:
        small = small_parameters(vectors, up_bias)
        wqkv, wo, wu, wd, vec, upb, tokh, coth, qkv, qkvh = gather_all(
            small, qkv_weight, out_weight, up_weight, down_weight, tokens, cotangent
        )
    else:
        whole = lambda a: lax.all_gather(a, AXES, axis=0, tiled=True)
        wqkv, wo, wu, wd = (whole(a) for a in (qkv_weight, out_weight, up_weight, down_weight))
        vec = jnp.stack([whole(a).astype(F32) for a in vectors])
        upb = jnp.broadcast_to(whole(up_bias).astype(F32)[None, :], (8, ff))
        n = lax.axis_size(AXES)
        up, down = [(i, i + 1) for i in range(n - 1)], [(i + 1, i) for i in range(n - 1)]
        side = lambda a: jnp.concatenate([lax.ppermute(a[a.shape[0] - LEFT :], AXES, up), lax.ppermute(a[:RIGHT], AXES, down)])
        tokh, coth = side(tokens), side(cotangent)
        qkv, qkvh = project(tokens, tokh, wqkv, vec)
    layer, dx, *grads = middle(
        packs, image_start, image_end, qkv, qkvh, tokens, tokh, cotangent, coth, wqkv, wo, wu, wd, vec, upb
    )
    if packs:
        gqkv, gwo, gwu, gwd, ups, *sums = finish(*scatter_all(*grads), width, ff)
    else:
        reduced = lambda a: lax.psum_scatter(a, AXES, scatter_dimension=0, tiled=True)
        sums, ups = reduced(grads[0].T).T, reduced(grads[1][0])
        gqkv, gwo, gwu, gwd = (reduced(a) for a in (grads[2], grads[3], grads[4], grads[5].T))
    return (
        layer, dx, gqkv, sums[0], sums[1], gwo, sums[2], gwu, ups, gwd, sums[3], sums[4], sums[5], sums[6], sums[7],
    )


def solution(mesh):
    both = P(AXES, None)
    one = P(AXES)
    in_specs = (both, both, one, one, both, one, one, both, one, both, one, both, one, one, one, one, one)
    out_specs = (both, both, both, one, one, both, one, both, one, both, one, one, one, one, one)
    return jax.shard_map(per_device, mesh=mesh, in_specs=in_specs, out_specs=out_specs, check_vma=False)
```
